128 devices in a mesh: train: 16 (over y_lo, z, core), query: 8 (over x, y_hi).
Axes of the slice: x: 4, y: 4 (y_hi: 2, y_lo: 2; y = y_hi * 2 + y_lo), z: 4, core: 2. Of those that a mesh axis runs over, the one named last changes fastest.
Arguments:
- train_losses: float32 [256, 131072], P('train', 'query'), may hold values from 0 to 16
- query_losses: float32 [256, 16384], P('train', 'query'), may hold values from 0 to 16
- chain_slots: int32 [32], replicated, may hold values from 0 to 31, as said below
- doc_lengths: int32 [128], replicated, may hold values from 1 to 4096, 131072 in all
Outputs:
- influence: float32 [128, 16384], P('train', 'query')
The draws below stay inside these ranges and needn't reach their ends.
Inputs may be any that keep to these rules, and one draw needn't show every extreme that they name: `chain_slots`: every chain appears exactly once. `doc_lengths`: the documents cover all 131072 train tokens in order.
All inputs are finite; a program needn't handle non-finite values.
Results may differ from the reference program's by a relative error of at most 0.00084.
Values may be sent and summed in bfloat16 or wider, within the bound.
No kernel may reach another device: no remote copies, remote signals or barrier semaphores. Data moves between devices by JAX's collectives and lax.ppermute only.
A program may use at most 64 MiB of HBM per device.

```python
import math
import jax
import jax.numpy as jnp
import numpy as np
from jax import lax

DRAWS = 256
CHAINS = 32
DOC_LEN = 1024
NTRAIN = 131072
NQ = 16384
DOCS = 128


factor_count = 16


def shared_factors(key):
    return jax.random.normal(jax.random.fold_in(key, 11), (DRAWS, factor_count), jnp.float32)


def slot_order(key):
    return jax.random.permutation(jax.random.fold_in(key, 13), CHAINS).astype(jnp.int32)


def token_losses(key, factors, token_total, region_size):
    key_list = jax.random.split(key, 5)
    base_loss = jax.random.uniform(key_list[0], (token_total,), jnp.float32, 1.0, 8.0)
    spread = jnp.exp(jax.random.uniform(key_list[1], (token_total,), jnp.float32, jnp.log(0.05), jnp.log(1.0)))
    jitter = jax.random.normal(key_list[2], (DRAWS, token_total), jnp.float32)
    region_count = (token_total + region_size - 1) // region_size
    regions = jax.random.normal(key_list[3], (region_count, factor_count), jnp.float32)
    loadings = regions[jnp.arange(token_total) // region_size] + 0.5 * jax.random.normal(key_list[4], (token_total, factor_count), jnp.float32)
    signal = jnp.dot(factors, loadings.T) * 0.5
    return jnp.clip(base_loss[None, :] + spread[None, :] * (signal + jitter), 0.0, 16.0)


def draw_train_losses(key, part):
    slot_chain = slot_order(key)
    factors = shared_factors(key).reshape(CHAINS, DRAWS // CHAINS, factor_count)[slot_chain].reshape(DRAWS, factor_count)
    return token_losses(jax.random.fold_in(key, 21), factors, NTRAIN, DOC_LEN)


def draw_query_losses(key, part):
    return token_losses(jax.random.fold_in(key, 31), shared_factors(key), NQ, 64)


def draw_chain_slots(key, part):
    return slot_order(key)


def split_up(count, total, reach, slope):
    loads = [(1 << 20) // math.isqrt(grade ** slope) + 1 for grade in range(2, count + 1)]
    surplus, counts = total - reach - (count - 1), [1] * (count - 1)
    while surplus > 0:
        movable = [i for i in range(count - 1) if counts[i] < reach]
        pool, remaining = sum([loads[i] for i in movable]), surplus
        for i in movable:
            more = min(reach - counts[i], max(1, remaining * loads[i] // pool), surplus)
            counts[i] = counts[i] + more
            surplus = surplus - more
    return np.array([reach] + counts)


def ragged_sizes(rng, number_of, total, bound, slope):
    if number_of == 2:
        one = jax.random.randint(rng, (), max(1, total - bound), min(bound, total - 1) + 1)
        return jnp.stack([one, total - one])
    tallies = jnp.asarray(split_up(number_of, total, bound, slope), jnp.int32)
    couples = (number_of - 1) // 2
    source_of, receiver = tallies[1:1 + 2 * couples:2], tallies[2:2 + 2 * couples:2]
    margin = jnp.minimum(source_of - 1, bound - receiver)
    shifted = jax.random.randint(jax.random.fold_in(rng, 1), (couples,), 0, 1 << 20) % (margin + 1)
    tallies = tallies.at[1:1 + 2 * couples:2].set(source_of - shifted).at[2:2 + 2 * couples:2].set(receiver + shifted)
    return tallies[jax.random.permutation(jax.random.fold_in(rng, 2), number_of)]


def setup_inputs(seed: int = 0) -> dict:
    keys = jax.random.split(jax.random.key(seed), 5)
    train_losses = draw_train_losses(jax.random.fold_in(keys[4], 71), 0)
    query_losses = draw_query_losses(jax.random.fold_in(keys[4], 71), 0)
    chain_slots = draw_chain_slots(jax.random.fold_in(keys[4], 71), 0)
    doc_lengths = ragged_sizes(keys[3], DOCS, NTRAIN, 4 * DOC_LEN, 2).astype(jnp.int32)
    return dict(train_losses=train_losses, query_losses=query_losses, chain_slots=chain_slots, doc_lengths=doc_lengths)


def reference(train_losses, query_losses, chain_slots, doc_lengths):
    highest = lax.Precision.HIGHEST
    train_mean = lax.optimization_barrier(jnp.sum(train_losses, axis=0)) / DRAWS
    train_centered = (train_losses - train_mean[None, :]).astype(jnp.bfloat16)
    query_mean = lax.optimization_barrier(jnp.sum(query_losses, axis=0)) / DRAWS
    query_centered = (query_losses - query_mean[None, :]).astype(jnp.bfloat16)
    per_chain = DRAWS // CHAINS
    query_paired = jnp.take(query_centered.reshape(CHAINS, per_chain, NQ), chain_slots, axis=0).reshape(DRAWS, NQ)
    train_wide = train_centered.astype(jnp.float32)
    query_wide = query_paired.astype(jnp.float32)
    train_scale = lax.rsqrt(lax.optimization_barrier(jnp.sum(train_wide * train_wide, axis=0)) / (DRAWS - 1) + 1e-06)
    query_scale = lax.rsqrt(lax.optimization_barrier(jnp.sum(query_wide * query_wide, axis=0)) / (DRAWS - 1) + 1e-06)
    doc_ends = jnp.cumsum(doc_lengths).astype(jnp.int32)
    doc_starts = (doc_ends - doc_lengths).astype(jnp.int32)
    block_rows = math.gcd(NTRAIN, 4096)
    block_count = NTRAIN // block_rows

    def one_block(running, block_index):
        offset = (block_index * block_rows).astype(jnp.int32)
        portion = lax.dynamic_slice_in_dim(train_centered, offset, block_rows, 1)
        scales = lax.dynamic_slice_in_dim(train_scale, offset, block_rows, 0)
        covariance = lax.dot_general(portion, query_paired, (((0,), (0,)), ((), ())), preferred_element_type=jnp.float32)
        correlation = covariance * scales[:, None] * query_scale[None, :] / (DRAWS - 1)
        signed = correlation * jnp.abs(correlation)
        positions = offset + jnp.arange(block_rows, dtype=jnp.int32)
        inside = (positions[:, None] >= doc_starts[None, :]) & (positions[:, None] < doc_ends[None, :])
        member = inside.astype(jnp.float32)
        added = lax.dot_general(member, signed, (((0,), (0,)), ((), ())), precision=highest, preferred_element_type=jnp.float32)
        return (running + added, None)
    start_value = jnp.zeros((DOCS, NQ), jnp.float32)
    pooled, _ = lax.scan(one_block, start_value, jnp.arange(block_count, dtype=jnp.int32))
    return pooled / doc_lengths[:, None].astype(jnp.float32)
```

```python
import jax
import jax.numpy as jnp
from jax import lax
from jax.experimental import pallas as pl
from jax.experimental.pallas import tpu as pltpu
from jax.sharding import Mesh
from jax.sharding import PartitionSpec as P

DRAWS = 256
CHAINS = 32
PER_CHAIN = DRAWS // CHAINS
EPS = 1e-06
DOCS = 128
DOC_OWN = 8
RUN = 1024
QPIECE = 128
TILE = 256
NBLK = 256
NTILE = 1024
NQ_HERE = 4096
NT_HERE = 4096

f32 = jnp.float32
bf16 = jnp.bfloat16


def params(mib=48):
    return pltpu.CompilerParams(vmem_limit_bytes=mib * 1024 * 1024)


def pack_body(train_ref, query_ref, out_ref):
    out_ref[0, :, :RUN] = train_ref[...]
    out_ref[0, :, RUN:] = query_ref[...]


def pack(train, query):
    rows = train.shape[0]
    return pl.pallas_call(
        pack_body,
        grid=(16,),
        in_specs=[
            pl.BlockSpec((rows, RUN), lambda i: (0, i)),
            pl.BlockSpec((rows, QPIECE), lambda i: (0, i)),
        ],
        out_specs=pl.BlockSpec((1, rows, RUN + QPIECE), lambda i: (i, 0, 0)),
        out_shape=jax.ShapeDtypeStruct((16, rows, RUN + QPIECE), f32),
        name="pack",
    )(train, query)


def centre_body(slots_ref, arr_ref, lo_ref, hi_ref, q_ref, qc_ref, qp_ref):
    def centred(j):
        block = arr_ref[:, :, j * 128 : (j + 1) * 128].reshape(DRAWS, 128)
        mean = jnp.sum(block, axis=0, keepdims=True) / DRAWS
        return (block - mean).astype(bf16).astype(f32)

    qc_ref[...] = centred(RUN // 128).reshape(CHAINS, PER_CHAIN, 128)
    for s in range(CHAINS):
        qp_ref[s] = qc_ref[slots_ref[s]]
    q_ref[...] = qp_ref[...].reshape(DRAWS, 128).astype(bf16)
    half = RUN // 2
    for j in range(RUN // 128):
        c = centred(j)
        scale = lax.rsqrt(jnp.sum(c * c, axis=0, keepdims=True) / (DRAWS - 1) + EPS)
        u = (c * scale).T.astype(bf16)
        ref = lo_ref if j * 128 < half else hi_ref
        o = j * 128 % half
        ref[o : o + 128, :] = u


def centre(slots, arr):
    half = jax.ShapeDtypeStruct((RUN // 2, DRAWS), bf16)
    return pl.pallas_call(
        centre_body,
        in_specs=[
            pl.BlockSpec(memory_space=pltpu.SMEM),
            pl.BlockSpec(memory_space=pltpu.VMEM),
        ],
        out_shape=(half, half, jax.ShapeDtypeStruct((DRAWS, QPIECE), bf16)),
        out_specs=[pl.BlockSpec(memory_space=pltpu.VMEM)] * 3,
        scratch_shapes=[
            pltpu.VMEM((CHAINS, PER_CHAIN, 128), f32),
            pltpu.VMEM((CHAINS, PER_CHAIN, 128), f32),
        ],
        compiler_params=params(),
        name="centre",
    )(slots, arr)


def pool_body(
    core_ref, bases_ref, starts_ref, ends_ref, first_ref, last_ref,
    t0, t1, t2, t3, t4, t5, t6, t7, qa_ref, qb_ref,
    send_ref, keep_ref,
    tok, qs, acc, tile_s, sem,
):
    core = core_ref[0]
    copies = []
    half = RUN // 2
    for i, t in enumerate((t0, t1, t2, t3, t4, t5, t6, t7)):
        copies.append(pltpu.make_async_copy(t, tok.at[pl.ds(i * half, half), :], sem))
    for i in range(16):
        ylz, yh = i // 2, i % 2
        for ref, c in ((qa_ref, core), (qb_ref, 1 - core)):
            col = pl.multiple_of((yh * 16 + ylz * 2 + c) * QPIECE, QPIECE)
            copies.append(pltpu.make_async_copy(ref.at[i], qs.at[:, pl.ds(col, QPIECE)], sem))
    for copy in copies:
        copy.start()
    acc[...] = jnp.zeros_like(acc)
    for copy in copies:
        copy.wait()

    def row_of(k):
        owner = k // DOC_OWN
        keep = jnp.where(owner % 2 == core, 1, 0)
        return keep * (DOCS // 2) + owner // 2 * DOC_OWN + k % DOC_OWN

    @pl.loop(0, NQ_HERE // NTILE)
    def _(n):
        cols = pl.multiple_of(n * NTILE, NTILE)

        @pl.loop(0, NT_HERE // TILE)
        def _(i):
            rows = pl.multiple_of(i * TILE, TILE)
            first = first_ref[i]
            last = last_ref[i]

            @pl.when(first == last)
            def _():
                lhs = tok[pl.ds(rows, TILE), :]
                row = row_of(first)
                for b in range(NTILE // NBLK):
                    where = pl.ds(cols + b * NBLK, NBLK)
                    s = jnp.dot(lhs, qs[:, where], preferred_element_type=f32)
                    total = jnp.sum(s * jnp.abs(s), axis=0, keepdims=True)
                    acc[pl.ds(row, 1), where] += total

            @pl.when(first != last)
            def _():
                lhs = tok[pl.ds(rows, TILE), :]
                for b in range(NTILE // NBLK):
                    tile_s[:, b * NBLK : (b + 1) * NBLK] = jnp.dot(
                        lhs, qs[:, pl.ds(cols + b * NBLK, NBLK)], preferred_element_type=f32
                    )
                base = bases_ref[i]

                def one_doc(k, _):
                    begin = jnp.maximum(starts_ref[k] - base, 0)
                    end = jnp.minimum(ends_ref[k] - base, TILE)

                    def one_group(g, total):
                        o = pl.multiple_of(g * 8, 8)
                        s = tile_s[pl.ds(o, 8), :]
                        at = lax.broadcasted_iota(jnp.int32, s.shape, 0) + o
                        inside = (at >= begin) & (at < end)
                        return total + jnp.where(inside, s * jnp.abs(s), 0.0)

                    total = lax.fori_loop(
                        begin // 8, (end + 7) // 8, one_group, jnp.zeros((8, NTILE), f32)
                    )
                    acc[pl.ds(row_of(k), 1), pl.ds(cols, NTILE)] += jnp.sum(
                        total, axis=0, keepdims=True
                    )
                    return 0

                lax.fori_loop(first, last + 1, one_doc, 0)

    send_ref[...] = acc[: DOCS // 2, :]
    keep_ref[...] = acc[DOCS // 2 :, :]


def pool(core, bases, starts, ends, first, last, tokens, qa, qb):
    smem = pl.BlockSpec(memory_space=pltpu.SMEM)
    anyspace = pl.BlockSpec(memory_space=pl.ANY)
    out = jax.ShapeDtypeStruct((DOCS // 2, NQ_HERE), f32)
    return pl.pallas_call(
        pool_body,
        in_specs=[smem] * 6 + [anyspace] * 10,
        out_shape=(out, out),
        out_specs=[pl.BlockSpec(memory_space=pltpu.VMEM)] * 2,
        scratch_shapes=[
            pltpu.VMEM((NT_HERE, DRAWS), bf16),
            pltpu.VMEM((DRAWS, NQ_HERE), bf16),
            pltpu.VMEM((DOCS, NQ_HERE), f32),
            pltpu.VMEM((TILE, NTILE), f32),
            pltpu.SemaphoreType.DMA,
        ],
        compiler_params=params(),
        cost_estimate=pl.CostEstimate(
            flops=2 * NT_HERE * NQ_HERE * DRAWS, bytes_accessed=6 << 20, transcendentals=0
        ),
        name="pool",
    )(core, bases, starts, ends, first, last, *tokens, qa, qb)


def finish_body(pieces_ref, q_ref, len_ref, out_ref):
    total = pieces_ref[0]
    for i in range(1, 16):
        total = total + pieces_ref[i]
    q = q_ref[...].astype(f32)
    scale = lax.rsqrt(jnp.sum(q * q, axis=0, keepdims=True) / (DRAWS - 1) + EPS) / (DRAWS - 1)
    out_ref[...] = total * (scale * scale) / len_ref[...]


def shift(value, axis, by):
    size = lax.axis_size(axis)
    return lax.ppermute(value, axis, [(i, (i + by) % size) for i in range(size)])


def shards(train_losses, query_losses, chain_slots, doc_lengths):
    core = lax.axis_index("c")
    yh = lax.axis_index("yh")
    x = lax.axis_index("x")
    t = (lax.axis_index("yl") * 4 + lax.axis_index("z")) * 2 + core

    doc_ends = jnp.cumsum(doc_lengths)
    doc_starts = doc_ends - doc_lengths

    packed = pack(train_losses, query_losses)
    arrived = lax.all_to_all(packed, ("yl", "z", "c"), split_axis=0, concat_axis=0, tiled=True)
    lo, hi, q_own = centre(chain_slots, arrived)

    left_lo = shift(lo, "x", 1)
    right_hi = shift(hi, "x", -1)
    left_hi = shift(hi, "x", 1)
    right_lo = shift(lo, "x", -1)
    far_lo = shift(left_lo, "x", 1)
    far_hi = shift(right_hi, "x", -1)

    qa = lax.all_to_all(
        jnp.broadcast_to(q_own, (16, *q_own.shape)), ("yl", "z", "yh"),
        split_axis=0, concat_axis=0, tiled=True,
    )
    qb = shift(qa, "c", 1)

    xs = jnp.stack([x, (x + 3) % 4, (x + 1) % 4, (x + 2) % 4])
    run_bases = (xs * 2 + yh) * (16 * RUN) + t * RUN
    bases = (run_bases[:, None] + jnp.arange(RUN // TILE, dtype=jnp.int32) * TILE).reshape(-1)
    first = jnp.sum(doc_ends[None, :] <= bases[:, None], axis=1, dtype=jnp.int32)
    last = jnp.sum(doc_ends[None, :] <= bases[:, None] + (TILE - 1), axis=1, dtype=jnp.int32)

    send, keep = pool(
        core.reshape(1), bases, doc_starts, doc_ends, first, last,
        (lo, hi, left_lo, left_hi, right_lo, right_hi, far_lo, far_hi), qa, qb,
    )
    other = shift(send, "c", 1)
    half = (keep + other).reshape(8, DOC_OWN, 2, 2048).transpose(0, 2, 1, 3)
    pieces = lax.all_to_all(
        half.reshape(16, DOC_OWN, 2048), ("yl", "z", "yh"), split_axis=0, concat_axis=0, tiled=True
    )

    mine = lax.dynamic_index_in_dim(qa.reshape(8, 2, DRAWS, QPIECE), yh, 1, keepdims=False)
    theirs = lax.dynamic_index_in_dim(qb.reshape(8, 2, DRAWS, QPIECE), yh, 1, keepdims=False)
    both = jnp.where(core == 0, jnp.stack([mine, theirs], 1), jnp.stack([theirs, mine], 1))
    q_mine = both.transpose(2, 0, 1, 3).reshape(DRAWS, 2048)
    lengths = lax.dynamic_slice_in_dim(doc_lengths, t * DOC_OWN, DOC_OWN, 0).astype(f32)
    return pl.pallas_call(
        finish_body,
        out_shape=jax.ShapeDtypeStruct((DOC_OWN, 2048), f32),
        compiler_params=params(),
        name="finish",
    )(pieces, q_mine, lengths[:, None])


def solution(mesh):
    fine = Mesh(mesh.devices.reshape(2, 4, 2, 4, 2), ("yl", "z", "c", "x", "yh"))
    split = P(("yl", "z", "c"), ("x", "yh"))
    return jax.shard_map(
        shards, mesh=fine, in_specs=(split, split, P(), P()), out_specs=split, check_vma=False
    )
```

```python
import jax
import jax.numpy as jnp
from jax import lax
from jax.experimental import pallas as pl
from jax.experimental.pallas import tpu as pltpu
from jax.sharding import Mesh
from jax.sharding import PartitionSpec as P

DRAWS = 256
CHAINS = 32
PER_CHAIN = DRAWS // CHAINS
EPS = 1e-06
DOCS = 128
DOC_OWN = 8
RUN = 1024
QPIECE = 128
TILE = 256
NBLK = 512
NTILE = 1024
NQ_HERE = 4096
NT_HERE = 4096

f32 = jnp.float32
bf16 = jnp.bfloat16


def params(mib=48):
    return pltpu.CompilerParams(vmem_limit_bytes=mib * 1024 * 1024)


def pack_body(train_ref, query_ref, out_ref):
    for i in range(16):
        out_ref[i, :, :RUN] = train_ref[:, i * RUN : (i + 1) * RUN]
        out_ref[i, :, RUN:] = query_ref[:, i * QPIECE : (i + 1) * QPIECE]


def pack(train, query):
    rows = train.shape[0]
    return pl.pallas_call(
        pack_body,
        in_specs=[pl.BlockSpec(memory_space=pltpu.VMEM)] * 2,
        out_specs=pl.BlockSpec(memory_space=pltpu.VMEM),
        out_shape=jax.ShapeDtypeStruct((16, rows, RUN + QPIECE), f32),
        compiler_params=params(16),
        name="pack",
    )(train, query)


def centre_body(slots_ref, arr_ref, u_ref, q_ref, qc_ref, qp_ref):
    def centred(j):
        block = arr_ref[:, :, j * 128 : (j + 1) * 128].reshape(DRAWS, 128)
        mean = jnp.sum(block, axis=0, keepdims=True) / DRAWS
        return (block - mean).astype(bf16).astype(f32)

    qc_ref[...] = centred(RUN // 128).reshape(CHAINS, PER_CHAIN, 128)
    for s in range(CHAINS):
        qp_ref[s] = qc_ref[slots_ref[s]]
    q_ref[...] = qp_ref[...].reshape(DRAWS, 128).astype(bf16)
    for j in range(RUN // 128):
        c = centred(j)
        scale = lax.rsqrt(jnp.sum(c * c, axis=0, keepdims=True) / (DRAWS - 1) + EPS)
        u_ref[j * 128 : (j + 1) * 128, :] = (c * scale).T.astype(bf16)


def centre(slots, arr):
    return pl.pallas_call(
        centre_body,
        in_specs=[
            pl.BlockSpec(memory_space=pltpu.SMEM),
            pl.BlockSpec(memory_space=pltpu.VMEM),
        ],
        out_shape=(
            jax.ShapeDtypeStruct((RUN, DRAWS), bf16),
            jax.ShapeDtypeStruct((DRAWS, QPIECE), bf16),
        ),
        out_specs=[pl.BlockSpec(memory_space=pltpu.VMEM)] * 2,
        scratch_shapes=[
            pltpu.VMEM((CHAINS, PER_CHAIN, 128), f32),
            pltpu.VMEM((CHAINS, PER_CHAIN, 128), f32),
        ],
        compiler_params=params(16),
        name="centre",
    )(slots, arr)


def pool_body(
    core_ref, bases_ref, starts_ref, ends_ref, first_ref, last_ref,
    own, left, right, far, qa_ref, qb_ref,
    send_ref, keep_ref,
    tok, qs, acc, tile_s,
):
    core = core_ref[0]
    at = 0
    for ref in (own, left, right, far):
        tok[at : at + ref.shape[0], :] = ref[...]
        at += ref.shape[0]
    for i in range(16):
        ylz, yh = i // 2, i % 2
        for ref, c in ((qa_ref, core), (qb_ref, 1 - core)):
            col = pl.multiple_of((yh * 16 + ylz * 2 + c) * QPIECE, QPIECE)
            qs[:, pl.ds(col, QPIECE)] = ref[i]
    acc[...] = jnp.zeros_like(acc)

    def row_of(k):
        owner = k // DOC_OWN
        keep = jnp.where(owner % 2 == core, 1, 0)
        return keep * (DOCS // 2) + owner // 2 * DOC_OWN + k % DOC_OWN

    @pl.loop(0, NT_HERE // TILE)
    def _(i):
        rows = pl.multiple_of(i * TILE, TILE)
        first = first_ref[i]
        last = last_ref[i]
        base = bases_ref[i]

        def products():
            lhs = tok[pl.ds(rows, TILE), :]
            for b in range(NQ_HERE // NBLK):
                where = slice(b * NBLK, (b + 1) * NBLK)
                yield where, jnp.dot(lhs, qs[:, where], preferred_element_type=f32)

        @pl.when(first == last)
        def _():
            row = row_of(first)
            for where, s in products():
                acc[pl.ds(row, 1), where] += jnp.sum(s * jnp.abs(s), axis=0, keepdims=True)

        @pl.when(first + 1 == last)
        def _():
            row = row_of(first)
            row_next = row_of(last)
            border = ends_ref[first] - base
            upper = lax.broadcasted_iota(jnp.int32, (TILE, NBLK), 0) < border
            for where, s in products():
                p = s * jnp.abs(s)
                p_upper = jnp.where(upper, p, 0.0)
                acc[pl.ds(row, 1), where] += jnp.sum(p_upper, axis=0, keepdims=True)
                acc[pl.ds(row_next, 1), where] += jnp.sum(p - p_upper, axis=0, keepdims=True)

        @pl.when(first + 1 < last)
        def _():
            for where, s in products():
                tile_s[:, where] = s

            def one_doc(k, _):
                begin = jnp.maximum(starts_ref[k] - base, 0)
                end = jnp.minimum(ends_ref[k] - base, TILE)
                row = row_of(k)

                @pl.loop(0, NQ_HERE // NTILE)
                def _(n):
                    cols = pl.ds(pl.multiple_of(n * NTILE, NTILE), NTILE)

                    def one_group(g, total):
                        o = pl.multiple_of(g * 8, 8)
                        s = tile_s[pl.ds(o, 8), cols]
                        at = lax.broadcasted_iota(jnp.int32, s.shape, 0) + o
                        inside = (at >= begin) & (at < end)
                        return total + jnp.where(inside, s * jnp.abs(s), 0.0)

                    total = lax.fori_loop(
                        begin // 8, (end + 7) // 8, one_group, jnp.zeros((8, NTILE), f32)
                    )
                    acc[pl.ds(row, 1), cols] += jnp.sum(total, axis=0, keepdims=True)

                return 0

            lax.fori_loop(first, last + 1, one_doc, 0)

    send_ref[...] = acc[: DOCS // 2, :]
    keep_ref[...] = acc[DOCS // 2 :, :]


def pool(core, bases, starts, ends, first, last, tokens, qa, qb):
    smem = pl.BlockSpec(memory_space=pltpu.SMEM)
    vmem = pl.BlockSpec(memory_space=pltpu.VMEM)
    out = jax.ShapeDtypeStruct((DOCS // 2, NQ_HERE), f32)
    return pl.pallas_call(
        pool_body,
        in_specs=[smem] * 6 + [vmem] * 6,
        out_shape=(out, out),
        out_specs=[vmem] * 2,
        scratch_shapes=[
            pltpu.VMEM((NT_HERE, DRAWS), bf16),
            pltpu.VMEM((DRAWS, NQ_HERE), bf16),
            pltpu.VMEM((DOCS, NQ_HERE), f32),
            pltpu.VMEM((TILE, NQ_HERE), f32),
        ],
        compiler_params=params(28),
        cost_estimate=pl.CostEstimate(
            flops=2 * NT_HERE * NQ_HERE * DRAWS, bytes_accessed=6 << 20, transcendentals=0
        ),
        name="pool",
    )(core, bases, starts, ends, first, last, *tokens, qa, qb)


def finish_body(pieces_ref, q_ref, len_ref, out_ref):
    total = pieces_ref[0]
    for i in range(1, 16):
        total = total + pieces_ref[i]
    q = q_ref[...].astype(f32)
    scale = lax.rsqrt(jnp.sum(q * q, axis=0, keepdims=True) / (DRAWS - 1) + EPS) / (DRAWS - 1)
    out_ref[...] = total * (scale * scale) / len_ref[...]


def shift(value, axis, by):
    size = lax.axis_size(axis)
    return lax.ppermute(value, axis, [(i, (i + by) % size) for i in range(size)])


def step(train_losses, query_losses, chain_slots, doc_lengths):
    core = lax.axis_index("c")
    yh = lax.axis_index("yh")
    x = lax.axis_index("x")
    t = (lax.axis_index("yl") * 4 + lax.axis_index("z")) * 2 + core

    doc_ends = jnp.cumsum(doc_lengths)
    doc_starts = doc_ends - doc_lengths

    packed = pack(train_losses, query_losses)
    arrived = lax.all_to_all(packed, ("yl", "z", "c"), split_axis=0, concat_axis=0, tiled=True)
    own, q_own = centre(chain_slots, arrived)

    left = shift(own, "x", 1)
    right = shift(own, "x", -1)
    far_lo = shift(left[: RUN // 2], "x", 1)
    far_hi = shift(right[RUN // 2 :], "x", -1)
    far = jnp.concatenate([far_lo, far_hi])

    copies = jnp.broadcast_to(q_own, (16, *q_own.shape))
    qa = lax.all_to_all(copies, ("yl", "z", "yh"), split_axis=0, concat_axis=0, tiled=True)
    qb = shift(qa, "c", 1)

    xs = jnp.stack([x, (x + 3) % 4, (x + 1) % 4, (x + 2) % 4])
    run_bases = (xs * 2 + yh) * (16 * RUN) + t * RUN
    bases = (run_bases[:, None] + jnp.arange(RUN // TILE, dtype=jnp.int32) * TILE).reshape(-1)
    first = jnp.sum(doc_ends[None, :] <= bases[:, None], axis=1, dtype=jnp.int32)
    last = jnp.sum(doc_ends[None, :] <= bases[:, None] + (TILE - 1), axis=1, dtype=jnp.int32)

    send, keep = pool(
        core.reshape(1), bases, doc_starts, doc_ends, first, last,
        (own, left, right, far), qa, qb,
    )
    other = shift(send, "c", 1)
    half = (keep + other).reshape(8, DOC_OWN, 2, 2048).transpose(0, 2, 1, 3)
    pieces = lax.all_to_all(
        half.reshape(16, DOC_OWN, 2048), ("yl", "z", "yh"), split_axis=0, concat_axis=0, tiled=True
    )

    mine = lax.dynamic_index_in_dim(qa.reshape(8, 2, DRAWS, QPIECE), yh, 1, keepdims=False)
    theirs = lax.dynamic_index_in_dim(qb.reshape(8, 2, DRAWS, QPIECE), yh, 1, keepdims=False)
    both = jnp.where(core == 0, jnp.stack([mine, theirs], 1), jnp.stack([theirs, mine], 1))
    q_mine = both.transpose(2, 0, 1, 3).reshape(DRAWS, 2048)
    lengths = lax.dynamic_slice_in_dim(doc_lengths, t * DOC_OWN, DOC_OWN, 0).astype(f32)
    return pl.pallas_call(
        finish_body,
        out_shape=jax.ShapeDtypeStruct((DOC_OWN, 2048), f32),
        compiler_params=params(16),
        name="finish",
    )(pieces, q_mine, lengths[:, None])


def solution(mesh):
    fine = Mesh(mesh.devices.reshape(2, 4, 2, 4, 2), ("yl", "z", "c", "x", "yh"))
    split = P(("yl", "z", "c"), ("x", "yh"))
    return jax.shard_map(
        step, mesh=fine, in_specs=(split, split, P(), P()), out_specs=split, check_vma=False
    )
```

```python
import jax
import jax.numpy as jnp
from jax import lax
from jax.experimental import pallas as pl
from jax.experimental.pallas import tpu as pltpu
from jax.sharding import Mesh
from jax.sharding import PartitionSpec as P

DRAWS = 256
CHAINS = 32
PER_CHAIN = DRAWS // CHAINS
EPS = 1e-06
DOCS = 128
DOC_OWN = 8
RUN = 1024
QPIECE = 128
TILE = 256
NBLK = 512
NTILE = 1024
NQ_HALF = 2048
PIECE = RUN + 256 + 3 * QPIECE
NT_HERE = 4096

f32 = jnp.float32
bf16 = jnp.bfloat16


def params(mib=48):
    return pltpu.CompilerParams(vmem_limit_bytes=mib * 1024 * 1024)


def terms(value):
    hi = value.astype(bf16).astype(f32)
    rest = value - hi
    mid = rest.astype(bf16).astype(f32)
    return hi, mid, rest - mid


def pack_body(train_ref, query_ref, out_ref):
    rows = train_ref.shape[0]
    for i in range(16):
        block = train_ref[:, i * RUN : (i + 1) * RUN]
        mean = jnp.sum(block, axis=0, keepdims=True) / rows
        out_ref[i, :, :RUN] = (block - mean).astype(bf16)
        stacked = jnp.concatenate([mean[:, j * 128 : (j + 1) * 128] for j in range(8)], axis=0)
        hi, mid, lo = terms(stacked)
        out_ref[i, :, RUN : RUN + 128] = jnp.concatenate([hi, mid], axis=0).astype(bf16)
        out_ref[i, :, RUN + 128 : RUN + 256] = jnp.concatenate([lo, lo], axis=0).astype(bf16)
        for k, term in enumerate(terms(query_ref[:, i * QPIECE : (i + 1) * QPIECE])):
            o = RUN + 256 + k * QPIECE
            out_ref[i, :, o : o + QPIECE] = term.astype(bf16)


def pack(train, query):
    return pl.pallas_call(
        pack_body,
        in_specs=[pl.BlockSpec(memory_space=pltpu.VMEM)] * 2,
        out_specs=pl.BlockSpec(memory_space=pltpu.VMEM),
        out_shape=jax.ShapeDtypeStruct((16, train.shape[0], PIECE), bf16),
        compiler_params=params(16),
        name="pack",
    )(train, query)


def centre_body(slots_ref, arr_ref, u_ref, q_ref, qc_ref, qp_ref, mean_ref):
    def part(o):
        return arr_ref[:, :, o : o + 128].astype(f32)

    o = RUN + 256
    query = ((part(o + 2 * QPIECE) + part(o + QPIECE)) + part(o)).reshape(DRAWS, QPIECE)
    mean = jnp.sum(query, axis=0, keepdims=True) / DRAWS
    qc = (query - mean).astype(bf16).astype(f32)
    qc_ref[...] = qc.reshape(CHAINS, PER_CHAIN, QPIECE)
    for s in range(CHAINS):
        qp_ref[s] = qc_ref[slots_ref[s]]
    q_ref[...] = qp_ref[...].reshape(DRAWS, QPIECE).astype(bf16)

    upper = part(RUN)
    mean_ref[...] = (part(RUN + 128)[:, :8] + upper[:, 8:]) + upper[:, :8]
    for j in range(RUN // 128):
        local = mean_ref[:, j : j + 1, :]
        offset = local - jnp.sum(local, axis=0, keepdims=True) / 16
        c = (part(j * 128) + offset).reshape(DRAWS, 128).astype(bf16).astype(f32)
        scale = lax.rsqrt(jnp.sum(c * c, axis=0, keepdims=True) / (DRAWS - 1) + EPS)
        u_ref[j * 128 : (j + 1) * 128, :] = (c * scale).T.astype(bf16)


def centre(slots, arr):
    return pl.pallas_call(
        centre_body,
        in_specs=[
            pl.BlockSpec(memory_space=pltpu.SMEM),
            pl.BlockSpec(memory_space=pltpu.VMEM),
        ],
        out_shape=(
            jax.ShapeDtypeStruct((RUN, DRAWS), bf16),
            jax.ShapeDtypeStruct((DRAWS, QPIECE), bf16),
        ),
        out_specs=[pl.BlockSpec(memory_space=pltpu.VMEM)] * 2,
        scratch_shapes=[
            pltpu.VMEM((CHAINS, PER_CHAIN, QPIECE), f32),
            pltpu.VMEM((CHAINS, PER_CHAIN, QPIECE), f32),
            pltpu.VMEM((16, 8, 128), f32),
        ],
        compiler_params=params(16),
        name="centre",
    )(slots, arr)


def pool_body(
    core_ref, bases_ref, starts_ref, ends_ref, first_ref, last_ref,
    own, left, right, far, q_ref,
    send_ref, keep_ref, weight_ref,
    tok, qs, acc, tile_s,
):
    core = core_ref[0]
    at = 0
    for ref in (own, left, right, far):
        tok[at : at + ref.shape[0], :] = ref[...]
        at += ref.shape[0]
    for i in range(16):
        o = (i % 2 * 8 + i // 2) * QPIECE
        block = q_ref[i]
        qs[:, o : o + QPIECE] = block
        wide = block.astype(f32)
        scale = lax.rsqrt(jnp.sum(wide * wide, axis=0, keepdims=True) / (DRAWS - 1) + EPS)
        weight_ref[:, o : o + QPIECE] = (scale / (DRAWS - 1)) * (scale / (DRAWS - 1))
    acc[...] = jnp.zeros_like(acc)

    def row_of(k):
        owner = k // DOC_OWN
        keep = jnp.where(owner % 2 == core, 1, 0)
        return keep * (DOCS // 2) + owner // 2 * DOC_OWN + k % DOC_OWN

    def products(rows):
        lhs = tok[pl.ds(rows, TILE), :]
        for b in range(NQ_HALF // NBLK):
            where = slice(b * NBLK, (b + 1) * NBLK)
            yield where, jnp.dot(lhs, qs[:, where], preferred_element_type=f32)

    def many(i, rows):
        for where, s in products(rows):
            tile_s[:, where] = s
        base = bases_ref[i]

        def one_doc(k, _):
            begin = jnp.maximum(starts_ref[k] - base, 0)
            end = jnp.minimum(ends_ref[k] - base, TILE)
            row = row_of(k)

            @pl.loop(0, NQ_HALF // NTILE)
            def _(n):
                cols = pl.ds(pl.multiple_of(n * NTILE, NTILE), NTILE)

                def one_group(g, total):
                    o = pl.multiple_of(g * 8, 8)
                    s = tile_s[pl.ds(o, 8), cols]
                    at = lax.broadcasted_iota(jnp.int32, s.shape, 0) + o
                    inside = (at >= begin) & (at < end)
                    return total + jnp.where(inside, s * jnp.abs(s), 0.0)

                total = lax.fori_loop(
                    begin // 8, (end + 7) // 8, one_group, jnp.zeros((8, NTILE), f32)
                )
                acc[pl.ds(row, 1), cols] += jnp.sum(total, axis=0, keepdims=True)

            return 0

        lax.fori_loop(first_ref[i], last_ref[i] + 1, one_doc, 0)

    @pl.loop(0, NT_HERE // TILE // 2)
    def _(pair):
        tiles = (2 * pair, 2 * pair + 1)
        rows = [pl.multiple_of(i * TILE, TILE) for i in tiles]
        extra = [last_ref[i] - first_ref[i] for i in tiles]
        most = jnp.maximum(extra[0], extra[1])

        @pl.when(most == 0)
        def _():
            for i, r in zip(tiles, rows):
                row = row_of(first_ref[i])
                for where, s in products(r):
                    acc[pl.ds(row, 1), where] += jnp.sum(s * jnp.abs(s), axis=0, keepdims=True)

        @pl.when(most == 1)
        def _():
            for i, r in zip(tiles, rows):
                row = row_of(first_ref[i])
                row_next = row_of(last_ref[i])
                border = ends_ref[first_ref[i]] - bases_ref[i]
                upper = lax.broadcasted_iota(jnp.int32, (TILE, NBLK), 0) < border
                for where, s in products(r):
                    p = s * jnp.abs(s)
                    p_upper = jnp.where(upper, p, 0.0)
                    acc[pl.ds(row, 1), where] += jnp.sum(p_upper, axis=0, keepdims=True)
                    acc[pl.ds(row_next, 1), where] += jnp.sum(p - p_upper, axis=0, keepdims=True)

        @pl.when(most > 1)
        def _():
            @pl.loop(2 * pair, 2 * pair + 2)
            def _(i):
                many(i, pl.multiple_of(i * TILE, TILE))

    send_ref[...] = acc[: DOCS // 2, :]
    keep_ref[...] = acc[DOCS // 2 :, :]


def pool(core, bases, starts, ends, first, last, tokens, q):
    smem = pl.BlockSpec(memory_space=pltpu.SMEM)
    vmem = pl.BlockSpec(memory_space=pltpu.VMEM)
    out = jax.ShapeDtypeStruct((DOCS // 2, NQ_HALF), f32)
    return pl.pallas_call(
        pool_body,
        in_specs=[smem] * 6 + [vmem] * 5,
        out_shape=(out, out, jax.ShapeDtypeStruct((1, NQ_HALF), f32)),
        out_specs=[vmem] * 3,
        scratch_shapes=[
            pltpu.VMEM((NT_HERE, DRAWS), bf16),
            pltpu.VMEM((DRAWS, NQ_HALF), bf16),
            pltpu.VMEM((DOCS, NQ_HALF), f32),
            pltpu.VMEM((TILE, NQ_HALF), f32),
        ],
        compiler_params=params(20),
        cost_estimate=pl.CostEstimate(
            flops=2 * NT_HERE * NQ_HALF * DRAWS, bytes_accessed=5 << 20, transcendentals=0
        ),
        name="pool",
    )(core, bases, starts, ends, first, last, *tokens, q)


def combine_body(keep_a, got_a, keep_b, got_b, out_ref):
    half = NQ_HALF // 2
    for d in range(16):
        ylz, yh = d // 2, d % 2
        r = slice(ylz * DOC_OWN, (ylz + 1) * DOC_OWN)
        c = slice(yh * half, (yh + 1) * half)
        out_ref[d, :, :half] = keep_a[r, c] + got_a[r, c]
        out_ref[d, :, half:] = keep_b[r, c] + got_b[r, c]


def combine(*arrays):
    return pl.pallas_call(
        combine_body,
        in_specs=[pl.BlockSpec(memory_space=pltpu.VMEM)] * 4,
        out_specs=pl.BlockSpec(memory_space=pltpu.VMEM),
        out_shape=jax.ShapeDtypeStruct((16, DOC_OWN, NQ_HALF), f32),
        compiler_params=params(16),
        name="combine",
    )(*arrays)


def finish_body(place_ref, pieces_ref, weight_a, weight_b, len_ref, out_ref):
    core = place_ref[0]
    yh = place_ref[1]
    total = pieces_ref[0]
    for i in range(1, 16):
        total = total + pieces_ref[i]
    total = total / len_ref[...]
    half = NQ_HALF // 2
    cols = pl.ds(pl.multiple_of(yh * half, half), half)
    for k, (weight, c) in enumerate(((weight_a, core), (weight_b, 1 - core))):
        part = total[:, k * half : (k + 1) * half] * weight[:, cols]
        for ylz in range(8):
            o = pl.multiple_of((ylz * 2 + c) * QPIECE, QPIECE)
            out_ref[:, pl.ds(o, QPIECE)] = part[:, ylz * QPIECE : (ylz + 1) * QPIECE]


def finish(place, pieces, weight_a, weight_b, lengths):
    vmem = pl.BlockSpec(memory_space=pltpu.VMEM)
    return pl.pallas_call(
        finish_body,
        in_specs=[pl.BlockSpec(memory_space=pltpu.SMEM)] + [vmem] * 4,
        out_specs=vmem,
        out_shape=jax.ShapeDtypeStruct((DOC_OWN, NQ_HALF), f32),
        compiler_params=params(16),
        name="finish",
    )(place, pieces, weight_a, weight_b, lengths)


def shift(value, axis, by):
    size = lax.axis_size(axis)
    return lax.ppermute(value, axis, [(i, (i + by) % size) for i in range(size)])


def step(train_losses, query_losses, chain_slots, doc_lengths):
    core = lax.axis_index("c")
    yh = lax.axis_index("yh")
    x = lax.axis_index("x")
    t = (lax.axis_index("yl") * 4 + lax.axis_index("z")) * 2 + core

    doc_ends = jnp.cumsum(doc_lengths)
    doc_starts = doc_ends - doc_lengths

    packed = pack(train_losses, query_losses)
    arrived = lax.all_to_all(packed, ("yl", "z", "c"), split_axis=0, concat_axis=0, tiled=True)
    own, q_own = centre(chain_slots, arrived)

    left = shift(own, "x", 1)
    right = shift(own, "x", -1)
    far_lo = shift(left[: RUN // 2], "x", 1)
    far_hi = shift(right[RUN // 2 :], "x", -1)
    far = jnp.concatenate([far_lo, far_hi])

    copies = jnp.broadcast_to(q_own, (16, *q_own.shape))
    qa = lax.all_to_all(copies, ("yl", "z", "yh"), split_axis=0, concat_axis=0, tiled=True)
    qb = shift(qa, "c", 1)

    xs = jnp.stack([x, (x + 3) % 4, (x + 1) % 4, (x + 2) % 4])
    run_bases = (xs * 2 + yh) * (16 * RUN) + t * RUN
    bases = (run_bases[:, None] + jnp.arange(RUN // TILE, dtype=jnp.int32) * TILE).reshape(-1)
    first = jnp.sum(doc_ends[None, :] <= bases[:, None], axis=1, dtype=jnp.int32)
    last = jnp.sum(doc_ends[None, :] <= bases[:, None] + (TILE - 1), axis=1, dtype=jnp.int32)

    where = (core.reshape(1), bases, doc_starts, doc_ends, first, last)
    tokens = (own, left, right, far)
    send_a, keep_a, weight_a = pool(*where, tokens, qa)
    cross_a = shift(send_a, "c", 1)
    send_b, keep_b, weight_b = pool(*where, tokens, qb)
    cross_b = shift(send_b, "c", 1)
    pieces = lax.all_to_all(
        combine(keep_a, cross_b, keep_b, cross_a), ("yl", "z", "yh"),
        split_axis=0, concat_axis=0, tiled=True,
    )
    lengths = lax.dynamic_slice_in_dim(doc_lengths, t * DOC_OWN, DOC_OWN, 0).astype(f32)
    return finish(jnp.stack([core, yh]), pieces, weight_a, weight_b, lengths[:, None])


def solution(mesh):
    fine = Mesh(mesh.devices.reshape(2, 4, 2, 4, 2), ("yl", "z", "c", "x", "yh"))
    split = P(("yl", "z", "c"), ("x", "yh"))
    return jax.shard_map(
        step, mesh=fine, in_specs=(split, split, P(), P()), out_specs=split, check_vma=False
    )
```

```python
import jax
import jax.numpy as jnp
from jax import lax
from jax.experimental import pallas as pl
from jax.experimental.pallas import tpu as pltpu
from jax.sharding import Mesh
from jax.sharding import PartitionSpec as P

DRAWS = 256
CHAINS = 32
PER_CHAIN = DRAWS // CHAINS
EPS = 1e-06
DOCS = 128
DOC_OWN = 8
RUN = 1024
QPIECE = 128
TILE = 256
NBLK = 512
BODY = 1024
NQ_HALF = 2048
PIECE = RUN + 256 + 3 * QPIECE
NT_HERE = 4096

f32 = jnp.float32
bf16 = jnp.bfloat16


def params(mib=48):
    return pltpu.CompilerParams(vmem_limit_bytes=mib * 1024 * 1024)


def terms(value):
    hi = value.astype(bf16).astype(f32)
    rest = value - hi
    mid = rest.astype(bf16).astype(f32)
    return hi, mid, rest - mid


def pack_body(train_ref, query_ref, out_ref):
    rows = train_ref.shape[0]
    for i in range(16):
        block = train_ref[:, i * RUN : (i + 1) * RUN]
        mean = jnp.sum(block, axis=0, keepdims=True) / rows
        out_ref[i, :, :RUN] = (block - mean).astype(bf16)
        stacked = jnp.concatenate([mean[:, j * 128 : (j + 1) * 128] for j in range(8)], axis=0)
        hi, mid, lo = terms(stacked)
        out_ref[i, :, RUN : RUN + 128] = jnp.concatenate([hi, mid], axis=0).astype(bf16)
        out_ref[i, :, RUN + 128 : RUN + 256] = jnp.concatenate([lo, lo], axis=0).astype(bf16)
        for k, term in enumerate(terms(query_ref[:, i * QPIECE : (i + 1) * QPIECE])):
            o = RUN + 256 + k * QPIECE
            out_ref[i, :, o : o + QPIECE] = term.astype(bf16)


def pack(train, query):
    return pl.pallas_call(
        pack_body,
        in_specs=[pl.BlockSpec(memory_space=pltpu.VMEM)] * 2,
        out_specs=pl.BlockSpec(memory_space=pltpu.VMEM),
        out_shape=jax.ShapeDtypeStruct((16, train.shape[0], PIECE), bf16),
        compiler_params=params(16),
        name="pack",
    )(train, query)


def centre_body(slots_ref, arr_ref, u_ref, q_ref, qc_ref, qp_ref, mean_ref):
    def part(o):
        return arr_ref[:, :, o : o + 128].astype(f32)

    o = RUN + 256
    query = ((part(o + 2 * QPIECE) + part(o + QPIECE)) + part(o)).reshape(DRAWS, QPIECE)
    mean = jnp.sum(query, axis=0, keepdims=True) / DRAWS
    qc = (query - mean).astype(bf16).astype(f32)
    qc_ref[...] = qc.reshape(CHAINS, PER_CHAIN, QPIECE)
    for s in range(CHAINS):
        qp_ref[s] = qc_ref[slots_ref[s]]
    paired = qp_ref[...].reshape(DRAWS, QPIECE).astype(bf16)
    for i in range(16):
        q_ref[i] = paired

    upper = part(RUN)
    mean_ref[...] = (part(RUN + 128)[:, :8] + upper[:, 8:]) + upper[:, :8]
    for j in range(RUN // 128):
        local = mean_ref[:, j : j + 1, :]
        offset = local - jnp.sum(local, axis=0, keepdims=True) / 16
        c = (part(j * 128) + offset).reshape(DRAWS, 128).astype(bf16).astype(f32)
        scale = lax.rsqrt(jnp.sum(c * c, axis=0, keepdims=True) / (DRAWS - 1) + EPS)
        u_ref[j * 128 : (j + 1) * 128, :] = (c * scale).T.astype(bf16)


def centre(slots, arr):
    return pl.pallas_call(
        centre_body,
        in_specs=[
            pl.BlockSpec(memory_space=pltpu.SMEM),
            pl.BlockSpec(memory_space=pltpu.VMEM),
        ],
        out_shape=(
            jax.ShapeDtypeStruct((RUN, DRAWS), bf16),
            jax.ShapeDtypeStruct((16, DRAWS, QPIECE), bf16),
        ),
        out_specs=[pl.BlockSpec(memory_space=pltpu.VMEM)] * 2,
        scratch_shapes=[
            pltpu.VMEM((CHAINS, PER_CHAIN, QPIECE), f32),
            pltpu.VMEM((CHAINS, PER_CHAIN, QPIECE), f32),
            pltpu.VMEM((16, 8, 128), f32),
        ],
        compiler_params=params(16),
        name="centre",
    )(slots, arr)


def rows_kept(block, begin, end):
    at = lax.broadcasted_iota(jnp.int32, block.shape, 0)
    inside = (at >= begin) & (at < end)
    return jnp.where(inside, block.astype(f32), 0.0).astype(bf16)


def pool_first_body(core_ref, bases_ref, starts_ref, ends_ref, first_ref, main_ref, last_ref,
                    own, left, right, far, q_ref,
                    send_ref, keep_ref, weight_ref, tok, main_tok, qs, acc):
    i = 0
    for ref in (own, left, right, far):
        for r in range(0, RUN, TILE):
            block = ref[r : r + TILE, :]
            k = main_ref[i]
            tok[i * TILE : (i + 1) * TILE, :] = block
            main_tok[i * TILE : (i + 1) * TILE, :] = rows_kept(
                block, starts_ref[k] - bases_ref[i], ends_ref[k] - bases_ref[i]
            )
            i += 1
    pool_columns(core_ref, bases_ref, starts_ref, ends_ref, first_ref, main_ref, last_ref,
                 tok, main_tok, q_ref, send_ref, keep_ref, weight_ref, qs, acc)


def pool_columns(core_ref, bases_ref, starts_ref, ends_ref, first_ref, main_ref, last_ref,
                 tok, main_tok, q_ref, send_ref, keep_ref, weight_ref, qs, acc):
    core = core_ref[0]
    for i in range(16):
        o = (i % 2 * 8 + i // 2) * QPIECE
        block = q_ref[i]
        qs[:, o : o + QPIECE] = block
        wide = block.astype(f32)
        scale = lax.rsqrt(jnp.sum(wide * wide, axis=0, keepdims=True) / (DRAWS - 1) + EPS)
        weight_ref[:, o : o + QPIECE] = (scale / (DRAWS - 1)) * (scale / (DRAWS - 1))
    acc[...] = jnp.zeros_like(acc)

    def row_of(k):
        owner = k // DOC_OWN
        keep = jnp.where(owner % 2 == core, 1, 0)
        return keep * (DOCS // 2) + owner // 2 * DOC_OWN + k % DOC_OWN

    def add_sums(lhs, k):
        row = row_of(k)
        for b in range(NQ_HALF // NBLK):
            where = slice(b * NBLK, (b + 1) * NBLK)
            s = jnp.dot(lhs, qs[:, where], preferred_element_type=f32)
            acc[pl.ds(row, 1), where] += jnp.sum(s * jnp.abs(s), axis=0, keepdims=True)

    tiles = BODY // TILE

    @pl.loop(0, NT_HERE // BODY)
    def _(block):
        for j in range(tiles):
            i = block * tiles + j
            add_sums(main_tok[pl.ds(pl.multiple_of(i * TILE, TILE), TILE), :], main_ref[i])

    @pl.loop(0, NT_HERE // TILE)
    def _(i):
        @pl.when(first_ref[i] != last_ref[i])
        def _():
            base = bases_ref[i]
            main = main_ref[i]

            def one_doc(k, _):
                @pl.when(k != main)
                def _():
                    half = TILE // 2
                    o = jnp.where(k > main, half, 0)
                    rows = pl.multiple_of(i * TILE + o, half)
                    lhs = rows_kept(
                        tok[pl.ds(rows, half), :], starts_ref[k] - base - o, ends_ref[k] - base - o
                    )
                    add_sums(lhs, k)

                return 0

            lax.fori_loop(first_ref[i], last_ref[i] + 1, one_doc, 0)

    send_ref[...] = acc[: DOCS // 2, :]
    keep_ref[...] = acc[DOCS // 2 :, :]


def pool(where, tokens, q):
    smem = pl.BlockSpec(memory_space=pltpu.SMEM)
    vmem = pl.BlockSpec(memory_space=pltpu.VMEM)
    sums = jax.ShapeDtypeStruct((DOCS // 2, NQ_HALF), f32)
    shapes = [sums, sums, jax.ShapeDtypeStruct((1, NQ_HALF), f32)]
    is_first = len(tokens) == 4
    if is_first:
        shapes += [jax.ShapeDtypeStruct((NT_HERE, DRAWS), bf16)] * 2
    return pl.pallas_call(
        pool_first_body if is_first else pool_columns,
        in_specs=[smem] * len(where) + [vmem] * (len(tokens) + 1),
        out_shape=shapes,
        out_specs=[vmem] * len(shapes),
        scratch_shapes=[
            pltpu.VMEM((DRAWS, NQ_HALF), bf16),
            pltpu.VMEM((DOCS, NQ_HALF), f32),
        ],
        compiler_params=params(20),
        cost_estimate=pl.CostEstimate(
            flops=2 * NT_HERE * NQ_HALF * DRAWS, bytes_accessed=5 << 20, transcendentals=0
        ),
        name="pool",
    )(*where, *tokens, q)


def combine_body(keep_a, got_a, keep_b, got_b, out_ref):
    half = NQ_HALF // 2
    for d in range(16):
        ylz, yh = d // 2, d % 2
        r = slice(ylz * DOC_OWN, (ylz + 1) * DOC_OWN)
        c = slice(yh * half, (yh + 1) * half)
        out_ref[d, :, :half] = keep_a[r, c] + got_a[r, c]
        out_ref[d, :, half:] = keep_b[r, c] + got_b[r, c]


def combine(*arrays):
    return pl.pallas_call(
        combine_body,
        in_specs=[pl.BlockSpec(memory_space=pltpu.VMEM)] * 4,
        out_specs=pl.BlockSpec(memory_space=pltpu.VMEM),
        out_shape=jax.ShapeDtypeStruct((16, DOC_OWN, NQ_HALF), f32),
        compiler_params=params(16),
        name="combine",
    )(*arrays)


def finish_body(place_ref, pieces_ref, weight_a, weight_b, len_ref, out_ref):
    core = place_ref[0]
    yh = place_ref[1]
    total = pieces_ref[0]
    for i in range(1, 16):
        total = total + pieces_ref[i]
    total = total / len_ref[...]
    half = NQ_HALF // 2
    cols = pl.ds(pl.multiple_of(yh * half, half), half)
    for k, (weight, c) in enumerate(((weight_a, core), (weight_b, 1 - core))):
        part = total[:, k * half : (k + 1) * half] * weight[:, cols]
        for ylz in range(8):
            o = pl.multiple_of((ylz * 2 + c) * QPIECE, QPIECE)
            out_ref[:, pl.ds(o, QPIECE)] = part[:, ylz * QPIECE : (ylz + 1) * QPIECE]


def finish(place, pieces, weight_a, weight_b, lengths):
    vmem = pl.BlockSpec(memory_space=pltpu.VMEM)
    return pl.pallas_call(
        finish_body,
        in_specs=[pl.BlockSpec(memory_space=pltpu.SMEM)] + [vmem] * 4,
        out_specs=vmem,
        out_shape=jax.ShapeDtypeStruct((DOC_OWN, NQ_HALF), f32),
        compiler_params=params(16),
        name="finish",
    )(place, pieces, weight_a, weight_b, lengths)


def shift(value, axis, by):
    size = lax.axis_size(axis)
    return lax.ppermute(value, axis, [(i, (i + by) % size) for i in range(size)])


def step(train_losses, query_losses, chain_slots, doc_lengths):
    core = lax.axis_index("c")
    yh = lax.axis_index("yh")
    x = lax.axis_index("x")
    t = (lax.axis_index("yl") * 4 + lax.axis_index("z")) * 2 + core

    packed = pack(train_losses, query_losses)
    arrived = lax.all_to_all(packed, ("yl", "z", "c"), split_axis=0, concat_axis=0, tiled=True)
    own, copies = centre(chain_slots, arrived)

    left = shift(own, "x", 1)
    right = shift(own, "x", -1)
    far_lo = shift(left[: RUN // 2], "x", 1)
    far_hi = shift(right[RUN // 2 :], "x", -1)
    far = jnp.concatenate([far_lo, far_hi])

    qa = lax.all_to_all(copies, ("yl", "z", "yh"), split_axis=0, concat_axis=0, tiled=True)
    qb = shift(qa, "c", 1)

    doc_ends = jnp.cumsum(doc_lengths)
    doc_starts = doc_ends - doc_lengths
    xs = jnp.stack([x, (x + 3) % 4, (x + 1) % 4, (x + 2) % 4])
    run_bases = (xs * 2 + yh) * (16 * RUN) + t * RUN
    bases = (run_bases[:, None] + jnp.arange(RUN // TILE, dtype=jnp.int32) * TILE).reshape(-1)
    spots = jnp.stack([bases, bases + TILE // 2, bases + (TILE - 1)])
    first, main, last = jnp.sum(
        doc_ends[None, None, :] <= spots[:, :, None], axis=2, dtype=jnp.int32
    )

    where = (core.reshape(1), bases, doc_starts, doc_ends, first, main, last)
    send_a, keep_a, weight_a, tok, main_tok = pool(where, (own, left, right, far), qa)
    cross_a = shift(send_a, "c", 1)
    send_b, keep_b, weight_b = pool(where, (tok, main_tok), qb)
    cross_b = shift(send_b, "c", 1)
    pieces = lax.all_to_all(
        combine(keep_a, cross_b, keep_b, cross_a), ("yl", "z", "yh"),
        split_axis=0, concat_axis=0, tiled=True,
    )
    lengths = lax.dynamic_slice_in_dim(doc_lengths, t * DOC_OWN, DOC_OWN, 0).astype(f32)
    return finish(jnp.stack([core, yh]), pieces, weight_a, weight_b, lengths[:, None])


def solution(mesh):
    fine = Mesh(mesh.devices.reshape(2, 4, 2, 4, 2), ("yl", "z", "c", "x", "yh"))
    split = P(("yl", "z", "c"), ("x", "yh"))
    return jax.shard_map(
        step, mesh=fine, in_specs=(split, split, P(), P()), out_specs=split, check_vma=False
    )
```

```python
import jax
import jax.numpy as jnp
from jax import lax
from jax.experimental import pallas as pl
from jax.experimental.pallas import tpu as pltpu
from jax.sharding import Mesh
from jax.sharding import PartitionSpec as P

DRAWS = 256
CHAINS = 32
PER_CHAIN = DRAWS // CHAINS
EPS = 1e-06
DOCS = 128
DOC_OWN = 8
RUN = 1024
QPIECE = 128
TILE = 256
NBLK = 512
BODY = 1024
PACK_MIB = 62
NQ_HALF = 2048
PIECE = RUN + 256 + 2 * QPIECE
NT_HERE = 4096

f32 = jnp.float32
bf16 = jnp.bfloat16


def params(mib=48):
    return pltpu.CompilerParams(vmem_limit_bytes=mib * 1024 * 1024)


def terms(value):
    hi = value.astype(bf16).astype(f32)
    rest = value - hi
    mid = rest.astype(bf16).astype(f32)
    return hi, mid, rest - mid


def pack_body(train_hbm, query_hbm, out_ref, train_ref, query_ref, sem):
    copies = [
        pltpu.make_async_copy(query_hbm, query_ref, sem.at[0]),
        pltpu.make_async_copy(train_hbm, train_ref, sem.at[1]),
    ]
    for copy in copies:
        copy.start()
    for copy in copies:
        copy.wait()
    rows = train_ref.shape[0]
    for i in range(16):
        block = train_ref[:, i * RUN : (i + 1) * RUN]
        mean = jnp.sum(block, axis=0, keepdims=True) / rows
        out_ref[i, :, :RUN] = (block - mean).astype(bf16)
        stacked = jnp.concatenate([mean[:, j * 128 : (j + 1) * 128] for j in range(8)], axis=0)
        hi, mid, lo = terms(stacked)
        block = query_ref[:, i * QPIECE : (i + 1) * QPIECE]
        mean = jnp.sum(block, axis=0, keepdims=True) / rows
        means = terms(mean)
        low = jnp.concatenate([lo, *means, jnp.zeros((5, 128), f32)], axis=0)
        o = RUN
        out_ref[i, :, o : o + 128] = jnp.concatenate([hi, mid], axis=0).astype(bf16)
        out_ref[i, :, o + 128 : o + 256] = low.astype(bf16)
        hi, mid, _ = terms(block - mean)
        out_ref[i, :, o + 256 : o + 384] = hi.astype(bf16)
        out_ref[i, :, o + 384 : o + 512] = mid.astype(bf16)


def pack(train, query):
    return pl.pallas_call(
        pack_body,
        in_specs=[pl.BlockSpec(memory_space=pltpu.HBM)] * 2,
        out_specs=pl.BlockSpec(memory_space=pltpu.VMEM),
        out_shape=jax.ShapeDtypeStruct((16, train.shape[0], PIECE), bf16),
        scratch_shapes=[
            pltpu.VMEM(train.shape, f32),
            pltpu.VMEM(query.shape, f32),
            pltpu.SemaphoreType.DMA((2,)),
        ],
        compiler_params=params(PACK_MIB),
        name="pack",
    )(train, query)


def centre_body(slots_ref, arr_ref, u_ref, q_ref, qc_ref, qp_ref, mean_ref):
    def part(o):
        return arr_ref[:, :, o : o + 128].astype(f32)

    low = part(RUN + 128)
    local = (low[:, 10:11] + low[:, 9:10]) + low[:, 8:9]
    offset = local - jnp.sum(local, axis=0, keepdims=True) / 16
    query = (part(RUN + 384) + part(RUN + 256)) + offset
    qc = query.reshape(DRAWS, QPIECE).astype(bf16).astype(f32)
    qc_ref[...] = qc.reshape(CHAINS, PER_CHAIN, QPIECE)
    for s in range(CHAINS):
        qp_ref[s] = qc_ref[slots_ref[s]]
    paired = qp_ref[...].reshape(DRAWS, QPIECE).astype(bf16)
    for i in range(16):
        q_ref[i] = paired

    upper = part(RUN)
    mean_ref[...] = (low[:, :8] + upper[:, 8:]) + upper[:, :8]
    for j in range(RUN // 128):
        local = mean_ref[:, j : j + 1, :]
        offset = local - jnp.sum(local, axis=0, keepdims=True) / 16
        c = (part(j * 128) + offset).reshape(DRAWS, 128).astype(bf16).astype(f32)
        scale = lax.rsqrt(jnp.sum(c * c, axis=0, keepdims=True) / (DRAWS - 1) + EPS)
        u_ref[j * 128 : (j + 1) * 128, :] = (c * scale).T.astype(bf16)


def centre(slots, arr):
    return pl.pallas_call(
        centre_body,
        in_specs=[
            pl.BlockSpec(memory_space=pltpu.SMEM),
            pl.BlockSpec(memory_space=pltpu.VMEM),
        ],
        out_shape=(
            jax.ShapeDtypeStruct((RUN, DRAWS), bf16),
            jax.ShapeDtypeStruct((16, DRAWS, QPIECE), bf16),
        ),
        out_specs=[pl.BlockSpec(memory_space=pltpu.VMEM)] * 2,
        scratch_shapes=[
            pltpu.VMEM((CHAINS, PER_CHAIN, QPIECE), f32),
            pltpu.VMEM((CHAINS, PER_CHAIN, QPIECE), f32),
            pltpu.VMEM((16, 8, 128), f32),
        ],
        compiler_params=params(16),
        name="centre",
    )(slots, arr)


def rows_kept(block, begin, end):
    at = lax.broadcasted_iota(jnp.int32, block.shape, 0)
    inside = (at >= begin) & (at < end)
    return jnp.where(inside, block.astype(f32), 0.0).astype(bf16)


def pool_first_body(core_ref, bases_ref, starts_ref, ends_ref, first_ref, main_ref, last_ref,
                    own, left, right, far, q_ref,
                    send_ref, keep_ref, weight_ref, tok, main_tok, qs, acc):
    i = 0
    for ref in (own, left, right, far):
        for r in range(0, RUN, TILE):
            block = ref[r : r + TILE, :]
            k = main_ref[i]
            tok[i * TILE : (i + 1) * TILE, :] = block
            main_tok[i * TILE : (i + 1) * TILE, :] = rows_kept(
                block, starts_ref[k] - bases_ref[i], ends_ref[k] - bases_ref[i]
            )
            i += 1
    pool_columns(core_ref, bases_ref, starts_ref, ends_ref, first_ref, main_ref, last_ref,
                 tok, main_tok, q_ref, send_ref, keep_ref, weight_ref, qs, acc)


def pool_columns(core_ref, bases_ref, starts_ref, ends_ref, first_ref, main_ref, last_ref,
                 tok, main_tok, q_ref, send_ref, keep_ref, weight_ref, qs, acc):
    core = core_ref[0]
    for i in range(16):
        o = (i % 2 * 8 + i // 2) * QPIECE
        block = q_ref[i]
        qs[:, o : o + QPIECE] = block
        wide = block.astype(f32)
        scale = lax.rsqrt(jnp.sum(wide * wide, axis=0, keepdims=True) / (DRAWS - 1) + EPS)
        weight_ref[:, o : o + QPIECE] = (scale / (DRAWS - 1)) * (scale / (DRAWS - 1))
    acc[...] = jnp.zeros_like(acc)

    def row_of(k):
        owner = k // DOC_OWN
        keep = jnp.where(owner % 2 == core, 1, 0)
        return keep * (DOCS // 2) + owner // 2 * DOC_OWN + k % DOC_OWN

    def add_sums(lhs, k):
        row = row_of(k)
        for b in range(NQ_HALF // NBLK):
            where = slice(b * NBLK, (b + 1) * NBLK)
            s = jnp.dot(lhs, qs[:, where], preferred_element_type=f32)
            acc[pl.ds(row, 1), where] += jnp.sum(s * jnp.abs(s), axis=0, keepdims=True)

    tiles = BODY // TILE

    @pl.loop(0, NT_HERE // BODY)
    def _(block):
        for j in range(tiles):
            i = block * tiles + j
            add_sums(main_tok[pl.ds(pl.multiple_of(i * TILE, TILE), TILE), :], main_ref[i])

    @pl.loop(0, NT_HERE // TILE)
    def _(i):
        @pl.when(first_ref[i] != last_ref[i])
        def _():
            base = bases_ref[i]
            main = main_ref[i]

            def one_doc(k, _):
                @pl.when(k != main)
                def _():
                    half = TILE // 2
                    o = jnp.where(k > main, half, 0)
                    rows = pl.multiple_of(i * TILE + o, half)
                    lhs = rows_kept(
                        tok[pl.ds(rows, half), :], starts_ref[k] - base - o, ends_ref[k] - base - o
                    )
                    add_sums(lhs, k)

                return 0

            lax.fori_loop(first_ref[i], last_ref[i] + 1, one_doc, 0)

    send_ref[...] = acc[: DOCS // 2, :]
    keep_ref[...] = acc[DOCS // 2 :, :]


def pool(where, tokens, q):
    smem = pl.BlockSpec(memory_space=pltpu.SMEM)
    vmem = pl.BlockSpec(memory_space=pltpu.VMEM)
    sums = jax.ShapeDtypeStruct((DOCS // 2, NQ_HALF), f32)
    shapes = [sums, sums, jax.ShapeDtypeStruct((1, NQ_HALF), f32)]
    is_first = len(tokens) == 4
    if is_first:
        shapes += [jax.ShapeDtypeStruct((NT_HERE, DRAWS), bf16)] * 2
    return pl.pallas_call(
        pool_first_body if is_first else pool_columns,
        in_specs=[smem] * len(where) + [vmem] * (len(tokens) + 1),
        out_shape=shapes,
        out_specs=[vmem] * len(shapes),
        scratch_shapes=[
            pltpu.VMEM((DRAWS, NQ_HALF), bf16),
            pltpu.VMEM((DOCS, NQ_HALF), f32),
        ],
        compiler_params=params(20),
        cost_estimate=pl.CostEstimate(
            flops=2 * NT_HERE * NQ_HALF * DRAWS, bytes_accessed=5 << 20, transcendentals=0
        ),
        name="pool",
    )(*where, *tokens, q)


def combine_body(keep_a, got_a, weight_a, keep_b, got_b, weight_b, out_ref):
    half = NQ_HALF // 2
    for d in range(16):
        ylz, yh = d // 2, d % 2
        r = slice(ylz * DOC_OWN, (ylz + 1) * DOC_OWN)
        c = slice(yh * half, (yh + 1) * half)
        out_ref[d, :, :half] = (keep_a[r, c] + got_a[r, c]) * weight_a[:, c]
        out_ref[d, :, half:] = (keep_b[r, c] + got_b[r, c]) * weight_b[:, c]


def combine(*arrays):
    return pl.pallas_call(
        combine_body,
        in_specs=[pl.BlockSpec(memory_space=pltpu.VMEM)] * 6,
        out_specs=pl.BlockSpec(memory_space=pltpu.VMEM),
        out_shape=jax.ShapeDtypeStruct((16, DOC_OWN, NQ_HALF), f32),
        compiler_params=params(16),
        name="combine",
    )(*arrays)


def finish_body(core_ref, total_ref, len_ref, out_ref):
    core = core_ref[0]
    total = total_ref[...] / len_ref[...]
    for k, c in enumerate((core, 1 - core)):
        for ylz in range(8):
            o = pl.multiple_of((ylz * 2 + c) * QPIECE, QPIECE)
            i = (k * 8 + ylz) * QPIECE
            out_ref[:, pl.ds(o, QPIECE)] = total[:, i : i + QPIECE]


def finish(core, total, lengths):
    vmem = pl.BlockSpec(memory_space=pltpu.VMEM)
    return pl.pallas_call(
        finish_body,
        in_specs=[pl.BlockSpec(memory_space=pltpu.SMEM)] + [vmem] * 2,
        out_specs=vmem,
        out_shape=jax.ShapeDtypeStruct((DOC_OWN, NQ_HALF), f32),
        compiler_params=params(16),
        name="finish",
    )(core, total, lengths)


def shift(value, axis, by):
    size = lax.axis_size(axis)
    return lax.ppermute(value, axis, [(i, (i + by) % size) for i in range(size)])


def step(train_losses, query_losses, chain_slots, doc_lengths):
    core = lax.axis_index("c")
    yh = lax.axis_index("yh")
    x = lax.axis_index("x")
    t = (lax.axis_index("yl") * 4 + lax.axis_index("z")) * 2 + core

    packed = pack(train_losses, query_losses)
    arrived = lax.all_to_all(packed, ("yl", "z", "c"), split_axis=0, concat_axis=0, tiled=True)
    own, copies = centre(chain_slots, arrived)

    left = shift(own, "x", 1)
    right = shift(own, "x", -1)
    far_lo = shift(left[: RUN // 2], "x", 1)
    far_hi = shift(right[RUN // 2 :], "x", -1)
    far = jnp.concatenate([far_lo, far_hi])

    qa = lax.all_to_all(copies, ("yl", "z", "yh"), split_axis=0, concat_axis=0, tiled=True)
    qb = shift(qa, "c", 1)

    doc_ends = jnp.cumsum(doc_lengths)
    doc_starts = doc_ends - doc_lengths
    xs = jnp.stack([x, (x + 3) % 4, (x + 1) % 4, (x + 2) % 4])
    run_bases = (xs * 2 + yh) * (16 * RUN) + t * RUN
    bases = (run_bases[:, None] + jnp.arange(RUN // TILE, dtype=jnp.int32) * TILE).reshape(-1)
    spots = jnp.stack([bases, bases + TILE // 2, bases + (TILE - 1)])
    first, main, last = jnp.sum(
        doc_ends[None, None, :] <= spots[:, :, None], axis=2, dtype=jnp.int32
    )

    where = (core.reshape(1), bases, doc_starts, doc_ends, first, main, last)
    send_a, keep_a, weight_a, tok, main_tok = pool(where, (own, left, right, far), qa)
    cross_a = shift(send_a, "c", 1)
    send_b, keep_b, weight_b = pool(where, (tok, main_tok), qb)
    cross_b = shift(send_b, "c", 1)
    sums = combine(keep_a, cross_b, weight_a, keep_b, cross_a, weight_b)
    pieces = lax.all_to_all(
        sums.astype(jnp.float16), ("yl", "z", "yh"), split_axis=0, concat_axis=0, tiled=True
    )
    total = jnp.sum(pieces.astype(f32), axis=0)
    lengths = lax.dynamic_slice_in_dim(doc_lengths, t * DOC_OWN, DOC_OWN, 0).astype(f32)
    return finish(core.reshape(1), total, lengths[:, None])


def solution(mesh):
    fine = Mesh(mesh.devices.reshape(2, 4, 2, 4, 2), ("yl", "z", "c", "x", "yh"))
    split = P(("yl", "z", "c"), ("x", "yh"))
    return jax.shard_map(
        step, mesh=fine, in_specs=(split, split, P(), P()), out_specs=split, check_vma=False
    )
```

```python
import jax
import jax.numpy as jnp
from jax import lax
from jax.experimental import pallas as pl
from jax.experimental.pallas import tpu as pltpu
from jax.sharding import Mesh
from jax.sharding import PartitionSpec as P

DRAWS = 256
CHAINS = 32
PER_CHAIN = DRAWS // CHAINS
EPS = 1e-06
DOCS = 128
DOC_OWN = 8
RUN = 1024
QPIECE = 128
TILE = 256
SUB = 128
PASSES = TILE // (SUB // 2)
NBLK = 512
BODY = 1024
PACK_MIB = 62
NQ_HALF = 2048
PIECE = RUN + 256 + 2 * QPIECE
NT_HERE = 4096

f32 = jnp.float32
bf16 = jnp.bfloat16


def params(mib=48):
    return pltpu.CompilerParams(vmem_limit_bytes=mib * 1024 * 1024)


def terms(value):
    hi = value.astype(bf16).astype(f32)
    rest = value - hi
    mid = rest.astype(bf16).astype(f32)
    return hi, mid, rest - mid


def pack_body(train_hbm, query_hbm, out_ref, train_ref, query_ref, sem):
    width = train_ref.shape[1] // 4
    copies = [pltpu.make_async_copy(query_hbm, query_ref, sem.at[4])]
    for i in range(4):
        cols = pl.ds(i * width, width)
        copies.append(pltpu.make_async_copy(train_hbm.at[:, cols], train_ref.at[:, cols], sem.at[i]))
    for copy in copies:
        copy.start()
    copies[0].wait()
    rows = train_ref.shape[0]
    for i in range(16):
        if i % 4 == 0:
            copies[1 + i // 4].wait()
        block = train_ref[:, i * RUN : (i + 1) * RUN]
        mean = jnp.sum(block, axis=0, keepdims=True) / rows
        out_ref[i, :, :RUN] = (block - mean).astype(bf16)
        stacked = jnp.concatenate([mean[:, j * 128 : (j + 1) * 128] for j in range(8)], axis=0)
        hi, mid, lo = terms(stacked)
        block = query_ref[:, i * QPIECE : (i + 1) * QPIECE]
        mean = jnp.sum(block, axis=0, keepdims=True) / rows
        means = terms(mean)
        low = jnp.concatenate([lo, *means, jnp.zeros((5, 128), f32)], axis=0)
        o = RUN
        out_ref[i, :, o : o + 128] = jnp.concatenate([hi, mid], axis=0).astype(bf16)
        out_ref[i, :, o + 128 : o + 256] = low.astype(bf16)
        hi, mid, _ = terms(block - mean)
        out_ref[i, :, o + 256 : o + 384] = hi.astype(bf16)
        out_ref[i, :, o + 384 : o + 512] = mid.astype(bf16)


def pack(train, query):
    return pl.pallas_call(
        pack_body,
        in_specs=[pl.BlockSpec(memory_space=pltpu.HBM)] * 2,
        out_specs=pl.BlockSpec(memory_space=pltpu.VMEM),
        out_shape=jax.ShapeDtypeStruct((16, train.shape[0], PIECE), bf16),
        scratch_shapes=[
            pltpu.VMEM(train.shape, f32),
            pltpu.VMEM(query.shape, f32),
            pltpu.SemaphoreType.DMA((5,)),
        ],
        compiler_params=params(PACK_MIB),
        name="pack",
    )(train, query)


def centre_body(slots_ref, arr_ref, u_ref, q_ref, qc_ref, qp_ref, mean_ref):
    def part(o):
        return arr_ref[:, :, o : o + 128].astype(f32)

    low = part(RUN + 128)
    local = (low[:, 10:11] + low[:, 9:10]) + low[:, 8:9]
    offset = local - jnp.sum(local, axis=0, keepdims=True) / 16
    query = (part(RUN + 384) + part(RUN + 256)) + offset
    qc = query.reshape(DRAWS, QPIECE).astype(bf16).astype(f32)
    qc_ref[...] = qc.reshape(CHAINS, PER_CHAIN, QPIECE)
    for s in range(CHAINS):
        qp_ref[s] = qc_ref[slots_ref[s]]
    paired = qp_ref[...].reshape(DRAWS, QPIECE).astype(bf16)
    for i in range(16):
        q_ref[i] = paired

    upper = part(RUN)
    mean_ref[...] = (low[:, :8] + upper[:, 8:]) + upper[:, :8]
    for j in range(RUN // 128):
        local = mean_ref[:, j : j + 1, :]
        offset = local - jnp.sum(local, axis=0, keepdims=True) / 16
        c = (part(j * 128) + offset).reshape(DRAWS, 128).astype(bf16).astype(f32)
        scale = lax.rsqrt(jnp.sum(c * c, axis=0, keepdims=True) / (DRAWS - 1) + EPS)
        u_ref[j * 128 : (j + 1) * 128, :] = (c * scale).T.astype(bf16)


def centre(slots, arr):
    return pl.pallas_call(
        centre_body,
        in_specs=[
            pl.BlockSpec(memory_space=pltpu.SMEM),
            pl.BlockSpec(memory_space=pltpu.VMEM),
        ],
        out_shape=(
            jax.ShapeDtypeStruct((RUN, DRAWS), bf16),
            jax.ShapeDtypeStruct((16, DRAWS, QPIECE), bf16),
        ),
        out_specs=[pl.BlockSpec(memory_space=pltpu.VMEM)] * 2,
        scratch_shapes=[
            pltpu.VMEM((CHAINS, PER_CHAIN, QPIECE), f32),
            pltpu.VMEM((CHAINS, PER_CHAIN, QPIECE), f32),
            pltpu.VMEM((16, 8, 128), f32),
        ],
        compiler_params=params(16),
        name="centre",
    )(slots, arr)


def rows_kept(block, begin, end):
    at = lax.broadcasted_iota(jnp.int32, block.shape, 0)
    inside = (at >= begin) & (at < end)
    return jnp.where(inside, block.astype(f32), 0.0).astype(bf16)


def pool_first_body(core_ref, bases_ref, starts_ref, ends_ref, first_ref, main_ref, last_ref,
                    own, left, right, far, q_ref,
                    send_ref, keep_ref, weight_ref, tok, main_tok, qs, acc, *lists):
    i = 0
    for ref in (own, left, right, far):
        for r in range(0, RUN, SUB):
            block = ref[r : r + SUB, :]
            k = main_ref[i]
            tok[i * SUB : (i + 1) * SUB, :] = block
            main_tok[i * SUB : (i + 1) * SUB, :] = rows_kept(
                block, starts_ref[k] - bases_ref[i], ends_ref[k] - bases_ref[i]
            )
            i += 1
    pool_columns(core_ref, bases_ref, starts_ref, ends_ref, first_ref, main_ref, last_ref,
                 tok, main_tok, q_ref, send_ref, keep_ref, weight_ref, qs, acc, *lists)


def pool_columns(core_ref, bases_ref, starts_ref, ends_ref, first_ref, main_ref, last_ref,
                 tok, main_tok, q_ref, send_ref, keep_ref, weight_ref, qs, acc,
                 picked, sub_list, doc_list):
    core = core_ref[0]
    for i in range(16):
        o = (i % 2 * 8 + i // 2) * QPIECE
        block = q_ref[i]
        qs[:, o : o + QPIECE] = block
        wide = block.astype(f32)
        scale = lax.rsqrt(jnp.sum(wide * wide, axis=0, keepdims=True) / (DRAWS - 1) + EPS)
        weight_ref[:, o : o + QPIECE] = (scale / (DRAWS - 1)) * (scale / (DRAWS - 1))
    acc[...] = jnp.zeros_like(acc)

    def row_of(k):
        owner = k // DOC_OWN
        keep = jnp.where(owner % 2 == core, 1, 0)
        return keep * (DOCS // 2) + owner // 2 * DOC_OWN + k % DOC_OWN

    def add_sums(lhs, docs):
        rows = [row_of(k) for k in docs]
        size = lhs.shape[0] // len(rows)
        for b in range(NQ_HALF // NBLK):
            where = slice(b * NBLK, (b + 1) * NBLK)
            s = jnp.dot(lhs, qs[:, where], preferred_element_type=f32)
            p = s * jnp.abs(s)
            for j, row in enumerate(rows):
                acc[pl.ds(row, 1), where] += jnp.sum(
                    p[j * size : (j + 1) * size], axis=0, keepdims=True
                )

    @pl.loop(0, NT_HERE // BODY)
    def _(block):
        for j in range(BODY // TILE):
            i = block * (BODY // TILE) + j
            lhs = main_tok[pl.ds(pl.multiple_of(i * TILE, TILE), TILE), :]
            add_sums(lhs, [main_ref[i * (TILE // SUB) + h] for h in range(TILE // SUB)])

    def list_docs(i, n):
        def list_doc(k, n):
            other = k != main_ref[i]

            @pl.when(other)
            def _():
                sub_list[n] = i
                doc_list[n] = k

            return n + other.astype(jnp.int32)

        return lax.fori_loop(first_ref[i], last_ref[i] + 1, list_doc, n)

    extra = lax.fori_loop(0, NT_HERE // SUB, list_docs, 0)
    half = SUB // 2

    @pl.loop(0, (extra + PASSES - 1) // PASSES)
    def _(g):
        docs = []
        for j in range(PASSES):
            e = g * PASSES + j
            at = jnp.minimum(e, extra - 1)
            i = sub_list[at]
            k = doc_list[at]
            o = jnp.where(k > main_ref[i], half, 0)
            base = bases_ref[i] + o
            end = jnp.where(e < extra, ends_ref[k] - base, 0)
            rows = pl.multiple_of(i * SUB + o, half)
            picked[j * half : (j + 1) * half, :] = rows_kept(
                tok[pl.ds(rows, half), :], starts_ref[k] - base, end
            )
            docs.append(k)
        add_sums(picked[...], docs)

    send_ref[...] = acc[: DOCS // 2, :]
    keep_ref[...] = acc[DOCS // 2 :, :]


def pool(where, tokens, q):
    smem = pl.BlockSpec(memory_space=pltpu.SMEM)
    vmem = pl.BlockSpec(memory_space=pltpu.VMEM)
    sums = jax.ShapeDtypeStruct((DOCS // 2, NQ_HALF), f32)
    shapes = [sums, sums, jax.ShapeDtypeStruct((1, NQ_HALF), f32)]
    is_first = len(tokens) == 4
    if is_first:
        shapes += [jax.ShapeDtypeStruct((NT_HERE, DRAWS), bf16)] * 2
    return pl.pallas_call(
        pool_first_body if is_first else pool_columns,
        in_specs=[smem] * len(where) + [vmem] * (len(tokens) + 1),
        out_shape=shapes,
        out_specs=[vmem] * len(shapes),
        scratch_shapes=[
            pltpu.VMEM((DRAWS, NQ_HALF), bf16),
            pltpu.VMEM((DOCS, NQ_HALF), f32),
            pltpu.VMEM((TILE, DRAWS), bf16),
            pltpu.SMEM((DOCS,), jnp.int32),
            pltpu.SMEM((DOCS,), jnp.int32),
        ],
        compiler_params=params(20),
        cost_estimate=pl.CostEstimate(
            flops=2 * NT_HERE * NQ_HALF * DRAWS, bytes_accessed=5 << 20, transcendentals=0
        ),
        name="pool",
    )(*where, *tokens, q)


def combine_body(keep_a, got_a, weight_a, keep_b, got_b, weight_b, out_ref):
    half = NQ_HALF // 2
    for d in range(16):
        ylz, yh = d // 2, d % 2
        r = slice(ylz * DOC_OWN, (ylz + 1) * DOC_OWN)
        c = slice(yh * half, (yh + 1) * half)
        out_ref[d, :, :half] = (keep_a[r, c] + got_a[r, c]) * weight_a[:, c]
        out_ref[d, :, half:] = (keep_b[r, c] + got_b[r, c]) * weight_b[:, c]


def combine(*arrays):
    return pl.pallas_call(
        combine_body,
        in_specs=[pl.BlockSpec(memory_space=pltpu.VMEM)] * 6,
        out_specs=pl.BlockSpec(memory_space=pltpu.VMEM),
        out_shape=jax.ShapeDtypeStruct((16, DOC_OWN, NQ_HALF), f32),
        compiler_params=params(16),
        name="combine",
    )(*arrays)


def finish_body(core_ref, total_ref, len_ref, out_ref):
    core = core_ref[0]
    total = total_ref[...] / len_ref[...]
    for k, c in enumerate((core, 1 - core)):
        for ylz in range(8):
            o = pl.multiple_of((ylz * 2 + c) * QPIECE, QPIECE)
            i = (k * 8 + ylz) * QPIECE
            out_ref[:, pl.ds(o, QPIECE)] = total[:, i : i + QPIECE]


def finish(core, total, lengths):
    vmem = pl.BlockSpec(memory_space=pltpu.VMEM)
    return pl.pallas_call(
        finish_body,
        in_specs=[pl.BlockSpec(memory_space=pltpu.SMEM)] + [vmem] * 2,
        out_specs=vmem,
        out_shape=jax.ShapeDtypeStruct((DOC_OWN, NQ_HALF), f32),
        compiler_params=params(16),
        name="finish",
    )(core, total, lengths)


def shift(value, axis, by):
    size = lax.axis_size(axis)
    return lax.ppermute(value, axis, [(i, (i + by) % size) for i in range(size)])


def step(train_losses, query_losses, chain_slots, doc_lengths):
    core = lax.axis_index("c")
    yh = lax.axis_index("yh")
    x = lax.axis_index("x")
    t = (lax.axis_index("yl") * 4 + lax.axis_index("z")) * 2 + core

    packed = pack(train_losses, query_losses)
    arrived = lax.all_to_all(packed, ("yl", "z", "c"), split_axis=0, concat_axis=0, tiled=True)
    own, copies = centre(chain_slots, arrived)

    left = shift(own, "x", 1)
    right = shift(own, "x", -1)
    far_lo = shift(left[: RUN // 2], "x", 1)
    far_hi = shift(right[RUN // 2 :], "x", -1)
    far = jnp.concatenate([far_lo, far_hi])

    qa = lax.all_to_all(copies, ("yl", "z", "yh"), split_axis=0, concat_axis=0, tiled=True)
    qb = shift(qa, "c", 1)

    doc_ends = jnp.cumsum(doc_lengths)
    doc_starts = doc_ends - doc_lengths
    xs = jnp.stack([x, (x + 3) % 4, (x + 1) % 4, (x + 2) % 4])
    run_bases = (xs * 2 + yh) * (16 * RUN) + t * RUN
    bases = (run_bases[:, None] + jnp.arange(RUN // SUB, dtype=jnp.int32) * SUB).reshape(-1)
    spots = jnp.stack([bases, bases + SUB // 2, bases + (SUB - 1)])
    first, main, last = jnp.sum(
        doc_ends[None, None, :] <= spots[:, :, None], axis=2, dtype=jnp.int32
    )

    where = (core.reshape(1), bases, doc_starts, doc_ends, first, main, last)
    send_a, keep_a, weight_a, tok, main_tok = pool(where, (own, left, right, far), qa)
    cross_a = shift(send_a, "c", 1)
    send_b, keep_b, weight_b = pool(where, (tok, main_tok), qb)
    cross_b = shift(send_b, "c", 1)
    sums = combine(keep_a, cross_b, weight_a, keep_b, cross_a, weight_b)
    pieces = lax.all_to_all(
        sums.astype(jnp.float16), ("yl", "z", "yh"), split_axis=0, concat_axis=0, tiled=True
    )
    total = jnp.sum(pieces.astype(f32), axis=0)
    lengths = lax.dynamic_slice_in_dim(doc_lengths, t * DOC_OWN, DOC_OWN, 0).astype(f32)
    return finish(core.reshape(1), total, lengths[:, None])


def solution(mesh):
    fine = Mesh(mesh.devices.reshape(2, 4, 2, 4, 2), ("yl", "z", "c", "x", "yh"))
    split = P(("yl", "z", "c"), ("x", "yh"))
    return jax.shard_map(
        step, mesh=fine, in_specs=(split, split, P(), P()), out_specs=split, check_vma=False
    )
```

```python
import jax
import jax.numpy as jnp
from jax import lax
from jax.experimental import pallas as pl
from jax.experimental.pallas import tpu as pltpu
from jax.sharding import Mesh
from jax.sharding import PartitionSpec as P

DRAWS = 256
CHAINS = 32
PER_CHAIN = DRAWS // CHAINS
EPS = 1e-06
DOCS = 128
DOC_OWN = 8
RUN = 1024
QPIECE = 128
TILE = 256
SUB = 128
PASSES = TILE // (SUB // 2)
NBLK = 512
BODY = 2048
PACK_MIB = 62
NQ_HALF = 2048
PIECE = RUN + 256 + 2 * QPIECE
NT_HERE = 4096

f32 = jnp.float32
bf16 = jnp.bfloat16


def params(mib=48):
    return pltpu.CompilerParams(vmem_limit_bytes=mib * 1024 * 1024)


def terms(value):
    hi = value.astype(bf16).astype(f32)
    rest = value - hi
    mid = rest.astype(bf16).astype(f32)
    return hi, mid, rest - mid


def pack_body(train_hbm, query_hbm, out_hbm, train_ref, query_ref, out_ref, sem, out_sem):
    width = train_ref.shape[1] // 4
    copies = [pltpu.make_async_copy(query_hbm, query_ref, sem.at[4])]
    for i in range(4):
        cols = pl.ds(i * width, width)
        copies.append(pltpu.make_async_copy(train_hbm.at[:, cols], train_ref.at[:, cols], sem.at[i]))
    for copy in copies:
        copy.start()
    out_copies = []
    for i in range(4):
        part = pl.ds(i * 4, 4)
        out_copies.append(pltpu.make_async_copy(out_ref.at[part], out_hbm.at[part], out_sem.at[i]))
    copies[0].wait()
    rows = train_ref.shape[0]
    for i in range(16):
        if i % 4 == 0:
            copies[1 + i // 4].wait()
        if i % 4 == 1 and i > 4:
            out_copies[i // 4 - 1].start()
        block = train_ref[:, i * RUN : (i + 1) * RUN]
        mean = jnp.sum(block, axis=0, keepdims=True) / rows
        out_ref[i, :, :RUN] = (block - mean).astype(bf16)
        stacked = jnp.concatenate([mean[:, j * 128 : (j + 1) * 128] for j in range(8)], axis=0)
        hi, mid, lo = terms(stacked)
        block = query_ref[:, i * QPIECE : (i + 1) * QPIECE]
        mean = jnp.sum(block, axis=0, keepdims=True) / rows
        means = terms(mean)
        low = jnp.concatenate([lo, *means, jnp.zeros((5, 128), f32)], axis=0)
        o = RUN
        out_ref[i, :, o : o + 128] = jnp.concatenate([hi, mid], axis=0).astype(bf16)
        out_ref[i, :, o + 128 : o + 256] = low.astype(bf16)
        hi, mid, _ = terms(block - mean)
        out_ref[i, :, o + 256 : o + 384] = hi.astype(bf16)
        out_ref[i, :, o + 384 : o + 512] = mid.astype(bf16)
    out_copies[3].start()
    for copy in out_copies:
        copy.wait()


def pack(train, query):
    return pl.pallas_call(
        pack_body,
        in_specs=[pl.BlockSpec(memory_space=pltpu.HBM)] * 2,
        out_specs=pl.BlockSpec(memory_space=pltpu.HBM),
        out_shape=jax.ShapeDtypeStruct((16, train.shape[0], PIECE), bf16),
        scratch_shapes=[
            pltpu.VMEM(train.shape, f32),
            pltpu.VMEM(query.shape, f32),
            pltpu.VMEM((16, train.shape[0], PIECE), bf16),
            pltpu.SemaphoreType.DMA((5,)),
            pltpu.SemaphoreType.DMA((4,)),
        ],
        compiler_params=params(PACK_MIB),
        name="pack",
    )(train, query)


def centre_body(slots_ref, arr_ref, u_ref, q_out, qc_ref, qp_ref, mean_ref, q_ref, sem):
    def part(o):
        return arr_ref[:, :, o : o + 128].astype(f32)

    low = part(RUN + 128)
    local = (low[:, 10:11] + low[:, 9:10]) + low[:, 8:9]
    offset = local - jnp.sum(local, axis=0, keepdims=True) / 16
    query = (part(RUN + 384) + part(RUN + 256)) + offset
    qc = query.reshape(DRAWS, QPIECE).astype(bf16).astype(f32)
    qc_ref[...] = qc.reshape(CHAINS, PER_CHAIN, QPIECE)
    for s in range(CHAINS):
        qp_ref[s] = qc_ref[slots_ref[s]]
    q_ref[...] = qp_ref[...].reshape(DRAWS, QPIECE).astype(bf16)

    upper = part(RUN)
    mean_ref[...] = (low[:, :8] + upper[:, 8:]) + upper[:, :8]
    for j in range(RUN // 128):
        local = mean_ref[:, j : j + 1, :]
        offset = local - jnp.sum(local, axis=0, keepdims=True) / 16
        c = (part(j * 128) + offset).reshape(DRAWS, 128).astype(bf16).astype(f32)
        scale = lax.rsqrt(jnp.sum(c * c, axis=0, keepdims=True) / (DRAWS - 1) + EPS)
        u_ref[j * 128 : (j + 1) * 128, :] = (c * scale).T.astype(bf16)
        if j == 0:
            copies = [
                pltpu.make_async_copy(q_ref, q_out.at[i], sem.at[i]) for i in range(16)
            ]
            for copy in copies:
                copy.start()
    for copy in copies:
        copy.wait()


def centre(slots, arr):
    return pl.pallas_call(
        centre_body,
        in_specs=[
            pl.BlockSpec(memory_space=pltpu.SMEM),
            pl.BlockSpec(memory_space=pltpu.VMEM),
        ],
        out_shape=(
            jax.ShapeDtypeStruct((RUN, DRAWS), bf16),
            jax.ShapeDtypeStruct((16, DRAWS, QPIECE), bf16),
        ),
        out_specs=[
            pl.BlockSpec(memory_space=pltpu.VMEM),
            pl.BlockSpec(memory_space=pltpu.HBM),
        ],
        scratch_shapes=[
            pltpu.VMEM((CHAINS, PER_CHAIN, QPIECE), f32),
            pltpu.VMEM((CHAINS, PER_CHAIN, QPIECE), f32),
            pltpu.VMEM((16, 8, 128), f32),
            pltpu.VMEM((DRAWS, QPIECE), bf16),
            pltpu.SemaphoreType.DMA((16,)),
        ],
        compiler_params=params(16),
        name="centre",
    )(slots, arr)


def rows_kept(block, begin, end):
    at = lax.broadcasted_iota(jnp.int32, block.shape, 0)
    inside = (at >= begin) & (at < end)
    return jnp.where(inside, block.astype(f32), 0.0).astype(bf16)


def pool_first_body(core_ref, bases_ref, starts_ref, ends_ref, first_ref, main_ref, last_ref,
                    own, left, right, far, q_ref,
                    send_ref, keep_ref, weight_ref, tok, main_tok, qs, acc, *lists):
    i = 0
    for ref in (own, left, right, far):
        for r in range(0, RUN, SUB):
            block = ref[r : r + SUB, :]
            k = main_ref[i]
            tok[i * SUB : (i + 1) * SUB, :] = block
            main_tok[i * SUB : (i + 1) * SUB, :] = rows_kept(
                block, starts_ref[k] - bases_ref[i], ends_ref[k] - bases_ref[i]
            )
            i += 1
    pool_columns(core_ref, bases_ref, starts_ref, ends_ref, first_ref, main_ref, last_ref,
                 tok, main_tok, q_ref, send_ref, keep_ref, weight_ref, qs, acc, *lists)


def pool_columns(core_ref, bases_ref, starts_ref, ends_ref, first_ref, main_ref, last_ref,
                 tok, main_tok, q_ref, send_ref, keep_ref, weight_ref, qs, acc,
                 picked, sub_list, doc_list):
    core = core_ref[0]
    for i in range(16):
        o = (i % 2 * 8 + i // 2) * QPIECE
        block = q_ref[i]
        qs[:, o : o + QPIECE] = block
        wide = block.astype(f32)
        scale = lax.rsqrt(jnp.sum(wide * wide, axis=0, keepdims=True) / (DRAWS - 1) + EPS)
        weight_ref[:, o : o + QPIECE] = (scale / (DRAWS - 1)) * (scale / (DRAWS - 1))
    acc[...] = jnp.zeros_like(acc)

    def row_of(k):
        owner = k // DOC_OWN
        keep = jnp.where(owner % 2 == core, 1, 0)
        return keep * (DOCS // 2) + owner // 2 * DOC_OWN + k % DOC_OWN

    def add_sums(lhs, docs):
        rows = [row_of(k) for k in docs]
        size = lhs.shape[0] // len(rows)
        for b in range(NQ_HALF // NBLK):
            where = slice(b * NBLK, (b + 1) * NBLK)
            s = jnp.dot(lhs, qs[:, where], preferred_element_type=f32)
            p = s * jnp.abs(s)
            for j, row in enumerate(rows):
                acc[pl.ds(row, 1), where] += jnp.sum(
                    p[j * size : (j + 1) * size], axis=0, keepdims=True
                )

    @pl.loop(0, NT_HERE // BODY)
    def _(block):
        for j in range(BODY // TILE):
            i = block * (BODY // TILE) + j
            lhs = main_tok[pl.ds(pl.multiple_of(i * TILE, TILE), TILE), :]
            add_sums(lhs, [main_ref[i * (TILE // SUB) + h] for h in range(TILE // SUB)])

    def list_docs(i, n):
        def list_doc(k, n):
            other = k != main_ref[i]

            @pl.when(other)
            def _():
                sub_list[n] = i
                doc_list[n] = k

            return n + other.astype(jnp.int32)

        return lax.fori_loop(first_ref[i], last_ref[i] + 1, list_doc, n)

    extra = lax.fori_loop(0, NT_HERE // SUB, list_docs, 0)
    half = SUB // 2

    @pl.loop(0, (extra + PASSES - 1) // PASSES)
    def _(g):
        docs = []
        for j in range(PASSES):
            e = g * PASSES + j
            at = jnp.minimum(e, extra - 1)
            i = sub_list[at]
            k = doc_list[at]
            o = jnp.where(k > main_ref[i], half, 0)
            base = bases_ref[i] + o
            end = jnp.where(e < extra, ends_ref[k] - base, 0)
            rows = pl.multiple_of(i * SUB + o, half)
            picked[j * half : (j + 1) * half, :] = rows_kept(
                tok[pl.ds(rows, half), :], starts_ref[k] - base, end
            )
            docs.append(k)
        add_sums(picked[...], docs)

    send_ref[...] = acc[: DOCS // 2, :]
    keep_ref[...] = acc[DOCS // 2 :, :]


def pool(where, tokens, q):
    smem = pl.BlockSpec(memory_space=pltpu.SMEM)
    vmem = pl.BlockSpec(memory_space=pltpu.VMEM)
    sums = jax.ShapeDtypeStruct((DOCS // 2, NQ_HALF), f32)
    shapes = [sums, sums, jax.ShapeDtypeStruct((1, NQ_HALF), f32)]
    is_first = len(tokens) == 4
    if is_first:
        shapes += [jax.ShapeDtypeStruct((NT_HERE, DRAWS), bf16)] * 2
    return pl.pallas_call(
        pool_first_body if is_first else pool_columns,
        in_specs=[smem] * len(where) + [vmem] * (len(tokens) + 1),
        out_shape=shapes,
        out_specs=[vmem] * len(shapes),
        scratch_shapes=[
            pltpu.VMEM((DRAWS, NQ_HALF), bf16),
            pltpu.VMEM((DOCS, NQ_HALF), f32),
            pltpu.VMEM((TILE, DRAWS), bf16),
            pltpu.SMEM((DOCS,), jnp.int32),
            pltpu.SMEM((DOCS,), jnp.int32),
        ],
        compiler_params=params(20),
        cost_estimate=pl.CostEstimate(
            flops=2 * NT_HERE * NQ_HALF * DRAWS, bytes_accessed=5 << 20, transcendentals=0
        ),
        name="pool",
    )(*where, *tokens, q)


def combine_body(keep_a, got_a, weight_a, keep_b, got_b, weight_b, out_ref):
    half = NQ_HALF // 2
    for d in range(16):
        ylz, yh = d // 2, d % 2
        r = slice(ylz * DOC_OWN, (ylz + 1) * DOC_OWN)
        c = slice(yh * half, (yh + 1) * half)
        out_ref[d, :, :half] = (keep_a[r, c] + got_a[r, c]) * weight_a[:, c]
        out_ref[d, :, half:] = (keep_b[r, c] + got_b[r, c]) * weight_b[:, c]


def combine(*arrays):
    return pl.pallas_call(
        combine_body,
        in_specs=[pl.BlockSpec(memory_space=pltpu.VMEM)] * 6,
        out_specs=pl.BlockSpec(memory_space=pltpu.VMEM),
        out_shape=jax.ShapeDtypeStruct((16, DOC_OWN, NQ_HALF), f32),
        compiler_params=params(16),
        name="combine",
    )(*arrays)


def finish_body(core_ref, total_ref, len_ref, out_ref):
    core = core_ref[0]
    total = total_ref[...] / len_ref[...]
    for k, c in enumerate((core, 1 - core)):
        for ylz in range(8):
            o = pl.multiple_of((ylz * 2 + c) * QPIECE, QPIECE)
            i = (k * 8 + ylz) * QPIECE
            out_ref[:, pl.ds(o, QPIECE)] = total[:, i : i + QPIECE]


def finish(core, total, lengths):
    vmem = pl.BlockSpec(memory_space=pltpu.VMEM)
    return pl.pallas_call(
        finish_body,
        in_specs=[pl.BlockSpec(memory_space=pltpu.SMEM)] + [vmem] * 2,
        out_specs=vmem,
        out_shape=jax.ShapeDtypeStruct((DOC_OWN, NQ_HALF), f32),
        compiler_params=params(16),
        name="finish",
    )(core, total, lengths)


def shift(value, axis, by):
    size = lax.axis_size(axis)
    return lax.ppermute(value, axis, [(i, (i + by) % size) for i in range(size)])


def step(train_losses, query_losses, chain_slots, doc_lengths):
    core = lax.axis_index("c")
    yh = lax.axis_index("yh")
    x = lax.axis_index("x")
    t = (lax.axis_index("yl") * 4 + lax.axis_index("z")) * 2 + core

    packed = pack(train_losses, query_losses)
    arrived = lax.all_to_all(packed, ("yl", "z", "c"), split_axis=0, concat_axis=0, tiled=True)
    own, copies = centre(chain_slots, arrived)

    left = shift(own, "x", 1)
    right = shift(own, "x", -1)
    far_lo = shift(left[: RUN // 2], "x", 1)
    far_hi = shift(right[RUN // 2 :], "x", -1)
    far = jnp.concatenate([far_lo, far_hi])

    qa = lax.all_to_all(copies, ("yl", "z", "yh"), split_axis=0, concat_axis=0, tiled=True)
    qb = shift(qa, "c", 1)

    doc_ends = jnp.cumsum(doc_lengths)
    doc_starts = doc_ends - doc_lengths
    xs = jnp.stack([x, (x + 3) % 4, (x + 1) % 4, (x + 2) % 4])
    run_bases = (xs * 2 + yh) * (16 * RUN) + t * RUN
    bases = (run_bases[:, None] + jnp.arange(RUN // SUB, dtype=jnp.int32) * SUB).reshape(-1)
    spots = jnp.stack([bases, bases + SUB // 2, bases + (SUB - 1)])
    first, main, last = jnp.sum(
        doc_ends[None, None, :] <= spots[:, :, None], axis=2, dtype=jnp.int32
    )

    where = (core.reshape(1), bases, doc_starts, doc_ends, first, main, last)
    send_a, keep_a, weight_a, tok, main_tok = pool(where, (own, left, right, far), qa)
    cross_a = shift(send_a, "c", 1)
    send_b, keep_b, weight_b = pool(where, (tok, main_tok), qb)
    cross_b = shift(send_b, "c", 1)
    sums = combine(keep_a, cross_b, weight_a, keep_b, cross_a, weight_b)
    pieces = lax.all_to_all(
        sums.astype(jnp.float16), ("yl", "z", "yh"), split_axis=0, concat_axis=0, tiled=True
    )
    total = jnp.sum(pieces.astype(f32), axis=0)
    lengths = lax.dynamic_slice_in_dim(doc_lengths, t * DOC_OWN, DOC_OWN, 0).astype(f32)
    return finish(core.reshape(1), total, lengths[:, None])


def solution(mesh):
    fine = Mesh(mesh.devices.reshape(2, 4, 2, 4, 2), ("yl", "z", "c", "x", "yh"))
    split = P(("yl", "z", "c"), ("x", "yh"))
    return jax.shard_map(
        step, mesh=fine, in_specs=(split, split, P(), P()), out_specs=split, check_vma=False
    )
```

```python
import jax
import jax.numpy as jnp
from jax import lax
from jax.experimental import pallas as pl
from jax.experimental.pallas import tpu as pltpu
from jax.sharding import Mesh
from jax.sharding import PartitionSpec as P

DRAWS = 256
CHAINS = 32
PER_CHAIN = DRAWS // CHAINS
EPS = 1e-06
DOCS = 128
DOC_OWN = 8
RUN = 1024
QPIECE = 128
TILE = 256
SUB = 128
PASSES = TILE // (SUB // 2)
NBLK = 512
BODY = 2048
PACK_MIB = 62
NQ_HALF = 2048
PIECE = RUN + 256 + 2 * QPIECE
NT_HERE = 4096

f32 = jnp.float32
bf16 = jnp.bfloat16


def params(mib=48):
    return pltpu.CompilerParams(vmem_limit_bytes=mib * 1024 * 1024)


def terms(value):
    hi = value.astype(bf16).astype(f32)
    rest = value - hi
    mid = rest.astype(bf16).astype(f32)
    return hi, mid, rest - mid


def pack_body(train_hbm, query_hbm, out_hbm, train_ref, query_ref, out_ref, sem, out_sem):
    width = train_ref.shape[1] // 4
    copies = [pltpu.make_async_copy(query_hbm, query_ref, sem.at[4])]
    for i in range(4):
        cols = pl.ds(i * width, width)
        copies.append(pltpu.make_async_copy(train_hbm.at[:, cols], train_ref.at[:, cols], sem.at[i]))
    for copy in copies:
        copy.start()
    out_copies = []
    for i in range(4):
        part = pl.ds(i * 4, 4)
        out_copies.append(pltpu.make_async_copy(out_ref.at[part], out_hbm.at[part], out_sem.at[i]))
    copies[0].wait()
    rows = train_ref.shape[0]
    for i in range(16):
        if i % 4 == 0:
            copies[1 + i // 4].wait()
        if i % 4 == 1 and i > 4:
            out_copies[i // 4 - 1].start()
        block = train_ref[:, i * RUN : (i + 1) * RUN]
        mean = jnp.sum(block, axis=0, keepdims=True) / rows
        out_ref[i, :, :RUN] = (block - mean).astype(bf16)
        stacked = jnp.concatenate([mean[:, j * 128 : (j + 1) * 128] for j in range(8)], axis=0)
        hi, mid, lo = terms(stacked)
        block = query_ref[:, i * QPIECE : (i + 1) * QPIECE]
        mean = jnp.sum(block, axis=0, keepdims=True) / rows
        means = terms(mean)
        low = jnp.concatenate([lo, *means, jnp.zeros((5, 128), f32)], axis=0)
        o = RUN
        out_ref[i, :, o : o + 128] = jnp.concatenate([hi, mid], axis=0).astype(bf16)
        out_ref[i, :, o + 128 : o + 256] = low.astype(bf16)
        hi, mid, _ = terms(block - mean)
        out_ref[i, :, o + 256 : o + 384] = hi.astype(bf16)
        out_ref[i, :, o + 384 : o + 512] = mid.astype(bf16)
    out_copies[3].start()
    for copy in out_copies:
        copy.wait()


def pack(train, query):
    return pl.pallas_call(
        pack_body,
        in_specs=[pl.BlockSpec(memory_space=pltpu.HBM)] * 2,
        out_specs=pl.BlockSpec(memory_space=pltpu.HBM),
        out_shape=jax.ShapeDtypeStruct((16, train.shape[0], PIECE), bf16),
        scratch_shapes=[
            pltpu.VMEM(train.shape, f32),
            pltpu.VMEM(query.shape, f32),
            pltpu.VMEM((16, train.shape[0], PIECE), bf16),
            pltpu.SemaphoreType.DMA((5,)),
            pltpu.SemaphoreType.DMA((4,)),
        ],
        compiler_params=params(PACK_MIB),
        name="pack",
    )(train, query)


def centre_body(slots_ref, arr_ref, u_ref, q_out, qc_ref, qp_ref, mean_ref, q_ref, sem):
    def part(o):
        return arr_ref[:, :, o : o + 128].astype(f32)

    low = part(RUN + 128)
    local = (low[:, 10:11] + low[:, 9:10]) + low[:, 8:9]
    offset = local - jnp.sum(local, axis=0, keepdims=True) / 16
    query = (part(RUN + 384) + part(RUN + 256)) + offset
    qc = query.reshape(DRAWS, QPIECE).astype(bf16).astype(f32)
    qc_ref[...] = qc.reshape(CHAINS, PER_CHAIN, QPIECE)
    for s in range(CHAINS):
        qp_ref[s] = qc_ref[slots_ref[s]]
    q_ref[...] = qp_ref[...].reshape(DRAWS, QPIECE).astype(bf16)

    upper = part(RUN)
    mean_ref[...] = (low[:, :8] + upper[:, 8:]) + upper[:, :8]
    for j in range(RUN // 128):
        local = mean_ref[:, j : j + 1, :]
        offset = local - jnp.sum(local, axis=0, keepdims=True) / 16
        c = (part(j * 128) + offset).reshape(DRAWS, 128).astype(bf16).astype(f32)
        scale = lax.rsqrt(jnp.sum(c * c, axis=0, keepdims=True) / (DRAWS - 1) + EPS)
        u_ref[j * 128 : (j + 1) * 128, :] = (c * scale).T.astype(bf16)
        if j == 0:
            copies = [
                pltpu.make_async_copy(q_ref, q_out.at[i], sem.at[i]) for i in range(16)
            ]
            for copy in copies:
                copy.start()
    for copy in copies:
        copy.wait()


def centre(slots, arr):
    return pl.pallas_call(
        centre_body,
        in_specs=[
            pl.BlockSpec(memory_space=pltpu.SMEM),
            pl.BlockSpec(memory_space=pltpu.VMEM),
        ],
        out_shape=(
            jax.ShapeDtypeStruct((RUN, DRAWS), bf16),
            jax.ShapeDtypeStruct((16, DRAWS, QPIECE), bf16),
        ),
        out_specs=[
            pl.BlockSpec(memory_space=pltpu.VMEM),
            pl.BlockSpec(memory_space=pltpu.HBM),
        ],
        scratch_shapes=[
            pltpu.VMEM((CHAINS, PER_CHAIN, QPIECE), f32),
            pltpu.VMEM((CHAINS, PER_CHAIN, QPIECE), f32),
            pltpu.VMEM((16, 8, 128), f32),
            pltpu.VMEM((DRAWS, QPIECE), bf16),
            pltpu.SemaphoreType.DMA((16,)),
        ],
        compiler_params=params(16),
        name="centre",
    )(slots, arr)


def rows_kept(block, begin, end):
    at = lax.broadcasted_iota(jnp.int32, block.shape, 0)
    inside = (at >= begin) & (at < end)
    return jnp.where(inside, block.astype(f32), 0.0).astype(bf16)


def docs_body(runs_ref, len_ref, bases_ref, starts_ref, ends_ref, first_ref, main_ref, last_ref):
    lengths = len_ref[...].astype(f32)
    row = lax.broadcasted_iota(jnp.int32, (DOCS, DOCS), 0)
    col = lax.broadcasted_iota(jnp.int32, (DOCS, DOCS), 1)
    column = jnp.sum(jnp.where(row == col, lengths, 0.0), axis=1, keepdims=True)
    ends_column = jnp.sum(jnp.where(col <= row, lengths, 0.0), axis=1, keepdims=True)
    ends = jnp.sum(jnp.where(row <= col, column, 0.0), axis=0, keepdims=True)
    ends_ref[...] = ends.astype(jnp.int32)
    starts_ref[...] = (ends - lengths).astype(jnp.int32)
    group = lax.broadcasted_iota(jnp.int32, (1, NT_HERE // SUB), 1)
    per_run = RUN // SUB
    base = group % per_run * SUB
    for i in range(4):
        base = base + jnp.where(group // per_run == i, runs_ref[i], 0)
    bases_ref[...] = base
    for ref, o in ((first_ref, 0), (main_ref, SUB // 2), (last_ref, SUB - 1)):
        before = ends_column <= (base + o).astype(f32)
        ref[...] = jnp.sum(jnp.where(before, 1.0, 0.0), axis=0, keepdims=True).astype(jnp.int32)


def docs_tables(runs, lengths):
    vmem = pl.BlockSpec(memory_space=pltpu.VMEM)
    groups = jax.ShapeDtypeStruct((1, NT_HERE // SUB), jnp.int32)
    table = jax.ShapeDtypeStruct((1, DOCS), jnp.int32)
    return pl.pallas_call(
        docs_body,
        in_specs=[pl.BlockSpec(memory_space=pltpu.SMEM), vmem],
        out_specs=[vmem] * 6,
        out_shape=[groups, table, table, groups, groups, groups],
        compiler_params=params(16),
        name="docs",
    )(runs, lengths)


def pool_first_body(core_ref, bases_ref, starts_ref, ends_ref, first_ref, main_ref, last_ref,
                    own, left, right, far, q_ref,
                    send_ref, keep_ref, weight_ref, tok, main_tok, qs, acc, *lists):
    i = 0
    for ref in (own, left, right, far):
        for r in range(0, RUN, SUB):
            block = ref[r : r + SUB, :]
            k = main_ref[0, i]
            tok[i * SUB : (i + 1) * SUB, :] = block
            main_tok[i * SUB : (i + 1) * SUB, :] = rows_kept(
                block, starts_ref[0, k] - bases_ref[0, i], ends_ref[0, k] - bases_ref[0, i]
            )
            i += 1
    pool_columns(core_ref, bases_ref, starts_ref, ends_ref, first_ref, main_ref, last_ref,
                 tok, main_tok, q_ref, send_ref, keep_ref, weight_ref, qs, acc, *lists)


def pool_columns(core_ref, bases_ref, starts_ref, ends_ref, first_ref, main_ref, last_ref,
                 tok, main_tok, q_ref, send_ref, keep_ref, weight_ref, qs, acc,
                 picked, sub_list, doc_list):
    core = core_ref[0]
    for i in range(16):
        o = (i % 2 * 8 + i // 2) * QPIECE
        block = q_ref[i]
        qs[:, o : o + QPIECE] = block
        wide = block.astype(f32)
        scale = lax.rsqrt(jnp.sum(wide * wide, axis=0, keepdims=True) / (DRAWS - 1) + EPS)
        weight_ref[:, o : o + QPIECE] = (scale / (DRAWS - 1)) * (scale / (DRAWS - 1))
    acc[...] = jnp.zeros_like(acc)

    def row_of(k):
        owner = k // DOC_OWN
        keep = jnp.where(owner % 2 == core, 1, 0)
        return keep * (DOCS // 2) + owner // 2 * DOC_OWN + k % DOC_OWN

    def add_sums(lhs, docs):
        rows = [row_of(k) for k in docs]
        size = lhs.shape[0] // len(rows)
        for b in range(NQ_HALF // NBLK):
            where = slice(b * NBLK, (b + 1) * NBLK)
            s = jnp.dot(lhs, qs[:, where], preferred_element_type=f32)
            p = s * jnp.abs(s)
            for j, row in enumerate(rows):
                acc[pl.ds(row, 1), where] += jnp.sum(
                    p[j * size : (j + 1) * size], axis=0, keepdims=True
                )

    @pl.loop(0, NT_HERE // BODY)
    def _(block):
        for j in range(BODY // TILE):
            i = block * (BODY // TILE) + j
            lhs = main_tok[pl.ds(pl.multiple_of(i * TILE, TILE), TILE), :]
            add_sums(lhs, [main_ref[0, i * (TILE // SUB) + h] for h in range(TILE // SUB)])

    def list_docs(i, n):
        def list_doc(k, n):
            other = k != main_ref[0, i]

            @pl.when(other)
            def _():
                sub_list[n] = i
                doc_list[n] = k

            return n + other.astype(jnp.int32)

        return lax.fori_loop(first_ref[0, i], last_ref[0, i] + 1, list_doc, n)

    extra = lax.fori_loop(0, NT_HERE // SUB, list_docs, 0)
    half = SUB // 2

    @pl.loop(0, (extra + PASSES - 1) // PASSES)
    def _(g):
        docs = []
        for j in range(PASSES):
            e = g * PASSES + j
            at = jnp.minimum(e, extra - 1)
            i = sub_list[at]
            k = doc_list[at]
            o = jnp.where(k > main_ref[0, i], half, 0)
            base = bases_ref[0, i] + o
            end = jnp.where(e < extra, ends_ref[0, k] - base, 0)
            rows = pl.multiple_of(i * SUB + o, half)
            picked[j * half : (j + 1) * half, :] = rows_kept(
                tok[pl.ds(rows, half), :], starts_ref[0, k] - base, end
            )
            docs.append(k)
        add_sums(picked[...], docs)

    send_ref[...] = acc[: DOCS // 2, :]
    keep_ref[...] = acc[DOCS // 2 :, :]


def pool(where, tokens, q):
    smem = pl.BlockSpec(memory_space=pltpu.SMEM)
    vmem = pl.BlockSpec(memory_space=pltpu.VMEM)
    sums = jax.ShapeDtypeStruct((DOCS // 2, NQ_HALF), f32)
    shapes = [sums, sums, jax.ShapeDtypeStruct((1, NQ_HALF), f32)]
    is_first = len(tokens) == 4
    if is_first:
        shapes += [jax.ShapeDtypeStruct((NT_HERE, DRAWS), bf16)] * 2
    return pl.pallas_call(
        pool_first_body if is_first else pool_columns,
        in_specs=[smem] * len(where) + [vmem] * (len(tokens) + 1),
        out_shape=shapes,
        out_specs=[vmem] * len(shapes),
        scratch_shapes=[
            pltpu.VMEM((DRAWS, NQ_HALF), bf16),
            pltpu.VMEM((DOCS, NQ_HALF), f32),
            pltpu.VMEM((TILE, DRAWS), bf16),
            pltpu.SMEM((DOCS,), jnp.int32),
            pltpu.SMEM((DOCS,), jnp.int32),
        ],
        compiler_params=params(20),
        cost_estimate=pl.CostEstimate(
            flops=2 * NT_HERE * NQ_HALF * DRAWS, bytes_accessed=5 << 20, transcendentals=0
        ),
        name="pool",
    )(*where, *tokens, q)


def combine_body(keep_a, got_a, weight_a, keep_b, got_b, weight_b, out_ref):
    half = NQ_HALF // 2
    for d in range(16):
        ylz, yh = d // 2, d % 2
        r = slice(ylz * DOC_OWN, (ylz + 1) * DOC_OWN)
        c = slice(yh * half, (yh + 1) * half)
        out_ref[d, :, :half] = (keep_a[r, c] + got_a[r, c]) * weight_a[:, c]
        out_ref[d, :, half:] = (keep_b[r, c] + got_b[r, c]) * weight_b[:, c]


def combine(*arrays):
    return pl.pallas_call(
        combine_body,
        in_specs=[pl.BlockSpec(memory_space=pltpu.VMEM)] * 6,
        out_specs=pl.BlockSpec(memory_space=pltpu.VMEM),
        out_shape=jax.ShapeDtypeStruct((16, DOC_OWN, NQ_HALF), f32),
        compiler_params=params(16),
        name="combine",
    )(*arrays)


def finish_body(core_ref, total_ref, len_ref, out_ref):
    core = core_ref[0]
    total = total_ref[...] / len_ref[...]
    for k, c in enumerate((core, 1 - core)):
        for ylz in range(8):
            o = pl.multiple_of((ylz * 2 + c) * QPIECE, QPIECE)
            i = (k * 8 + ylz) * QPIECE
            out_ref[:, pl.ds(o, QPIECE)] = total[:, i : i + QPIECE]


def finish(core, total, lengths):
    vmem = pl.BlockSpec(memory_space=pltpu.VMEM)
    return pl.pallas_call(
        finish_body,
        in_specs=[pl.BlockSpec(memory_space=pltpu.SMEM)] + [vmem] * 2,
        out_specs=vmem,
        out_shape=jax.ShapeDtypeStruct((DOC_OWN, NQ_HALF), f32),
        compiler_params=params(16),
        name="finish",
    )(core, total, lengths)


def shift(value, axis, by):
    size = lax.axis_size(axis)
    return lax.ppermute(value, axis, [(i, (i + by) % size) for i in range(size)])


def step(train_losses, query_losses, chain_slots, doc_lengths):
    core = lax.axis_index("c")
    yh = lax.axis_index("yh")
    x = lax.axis_index("x")
    t = (lax.axis_index("yl") * 4 + lax.axis_index("z")) * 2 + core

    packed = pack(train_losses, query_losses)
    arrived = lax.all_to_all(packed, ("yl", "z", "c"), split_axis=0, concat_axis=0, tiled=True)
    own, copies = centre(chain_slots, arrived)

    left = shift(own, "x", 1)
    right = shift(own, "x", -1)
    far_lo = shift(left[: RUN // 2], "x", 1)
    far_hi = shift(right[RUN // 2 :], "x", -1)
    far = jnp.concatenate([far_lo, far_hi])

    qa = lax.all_to_all(copies, ("yl", "z", "yh"), split_axis=0, concat_axis=0, tiled=True)
    qb = shift(qa, "c", 1)

    xs = jnp.stack([x, (x + 3) % 4, (x + 1) % 4, (x + 2) % 4])
    runs = (xs * 2 + yh) * (16 * RUN) + t * RUN
    tables = docs_tables(runs, doc_lengths.reshape(1, DOCS))
    bases, doc_starts, doc_ends, first, main, last = tables

    where = (core.reshape(1), bases, doc_starts, doc_ends, first, main, last)
    send_a, keep_a, weight_a, tok, main_tok = pool(where, (own, left, right, far), qa)
    cross_a = shift(send_a, "c", 1)
    send_b, keep_b, weight_b = pool(where, (tok, main_tok), qb)
    cross_b = shift(send_b, "c", 1)
    sums = combine(keep_a, cross_b, weight_a, keep_b, cross_a, weight_b)
    pieces = lax.all_to_all(
        sums.astype(jnp.float16), ("yl", "z", "yh"), split_axis=0, concat_axis=0, tiled=True
    )
    total = jnp.sum(pieces.astype(f32), axis=0)
    lengths = lax.dynamic_slice_in_dim(doc_lengths, t * DOC_OWN, DOC_OWN, 0).astype(f32)
    return finish(core.reshape(1), total, lengths[:, None])


def solution(mesh):
    fine = Mesh(mesh.devices.reshape(2, 4, 2, 4, 2), ("yl", "z", "c", "x", "yh"))
    split = P(("yl", "z", "c"), ("x", "yh"))
    return jax.shard_map(
        step, mesh=fine, in_specs=(split, split, P(), P()), out_specs=split, check_vma=False
    )
```

```python
import jax
import jax.numpy as jnp
from jax import lax
from jax.experimental import pallas as pl
from jax.experimental.pallas import tpu as pltpu
from jax.sharding import Mesh
from jax.sharding import PartitionSpec as P

DRAWS = 256
CHAINS = 32
PER_CHAIN = DRAWS // CHAINS
EPS = 1e-06
DOCS = 128
DOC_OWN = 8
RUN = 1024
QPIECE = 128
TILE = 256
SUB = 128
PASSES = TILE // (SUB // 2)
NBLK = 512
BODY = 2048
PACK_MIB = 62
NQ_HALF = 2048
PIECE = RUN + 256 + 2 * QPIECE
NT_HERE = 4096

f32 = jnp.float32
bf16 = jnp.bfloat16


def params(mib=48):
    return pltpu.CompilerParams(vmem_limit_bytes=mib * 1024 * 1024)


def terms(value):
    hi = value.astype(bf16).astype(f32)
    rest = value - hi
    mid = rest.astype(bf16).astype(f32)
    return hi, mid, rest - mid


def pack_body(train_hbm, query_hbm, out_hbm, train_ref, query_ref, out_ref, sem, out_sem):
    width = train_ref.shape[1] // 4
    copies = [pltpu.make_async_copy(query_hbm, query_ref, sem.at[4])]
    for i in range(4):
        cols = pl.ds(i * width, width)
        copies.append(pltpu.make_async_copy(train_hbm.at[:, cols], train_ref.at[:, cols], sem.at[i]))
    for copy in copies:
        copy.start()
    out_copies = []
    for i in range(4):
        part = pl.ds(i * 4, 4)
        out_copies.append(pltpu.make_async_copy(out_ref.at[part], out_hbm.at[part], out_sem.at[i]))
    copies[0].wait()
    rows = train_ref.shape[0]
    for i in range(16):
        if i % 4 == 0:
            copies[1 + i // 4].wait()
        if i % 4 == 1 and i > 4:
            out_copies[i // 4 - 1].start()
        block = train_ref[:, i * RUN : (i + 1) * RUN]
        mean = jnp.sum(block, axis=0, keepdims=True) / rows
        out_ref[i, :, :RUN] = (block - mean).astype(bf16)
        stacked = jnp.concatenate([mean[:, j * 128 : (j + 1) * 128] for j in range(8)], axis=0)
        hi, mid, lo = terms(stacked)
        block = query_ref[:, i * QPIECE : (i + 1) * QPIECE]
        mean = jnp.sum(block, axis=0, keepdims=True) / rows
        means = terms(mean)
        low = jnp.concatenate([lo, *means, jnp.zeros((5, 128), f32)], axis=0)
        o = RUN
        out_ref[i, :, o : o + 128] = jnp.concatenate([hi, mid], axis=0).astype(bf16)
        out_ref[i, :, o + 128 : o + 256] = low.astype(bf16)
        hi, mid, _ = terms(block - mean)
        out_ref[i, :, o + 256 : o + 384] = hi.astype(bf16)
        out_ref[i, :, o + 384 : o + 512] = mid.astype(bf16)
    out_copies[3].start()
    for copy in out_copies:
        copy.wait()


def pack(train, query):
    return pl.pallas_call(
        pack_body,
        in_specs=[pl.BlockSpec(memory_space=pltpu.HBM)] * 2,
        out_specs=pl.BlockSpec(memory_space=pltpu.HBM),
        out_shape=jax.ShapeDtypeStruct((16, train.shape[0], PIECE), bf16),
        scratch_shapes=[
            pltpu.VMEM(train.shape, f32),
            pltpu.VMEM(query.shape, f32),
            pltpu.VMEM((16, train.shape[0], PIECE), bf16),
            pltpu.SemaphoreType.DMA((5,)),
            pltpu.SemaphoreType.DMA((4,)),
        ],
        compiler_params=params(PACK_MIB),
        name="pack",
    )(train, query)


def centre_body(slots_ref, arr_ref, u_ref, q_out, qc_ref, qp_ref, mean_ref, q_ref, sem):
    def part(o):
        return arr_ref[:, :, o : o + 128].astype(f32)

    low = part(RUN + 128)
    local = (low[:, 10:11] + low[:, 9:10]) + low[:, 8:9]
    offset = local - jnp.sum(local, axis=0, keepdims=True) / 16
    query = (part(RUN + 384) + part(RUN + 256)) + offset
    qc = query.reshape(DRAWS, QPIECE).astype(bf16).astype(f32)
    qc_ref[...] = qc.reshape(CHAINS, PER_CHAIN, QPIECE)
    for s in range(CHAINS):
        qp_ref[s] = qc_ref[slots_ref[s]]
    q_ref[...] = qp_ref[...].reshape(DRAWS, QPIECE).astype(bf16)

    upper = part(RUN)
    mean_ref[...] = (low[:, :8] + upper[:, 8:]) + upper[:, :8]
    for j in range(RUN // 128):
        local = mean_ref[:, j : j + 1, :]
        offset = local - jnp.sum(local, axis=0, keepdims=True) / 16
        c = (part(j * 128) + offset).reshape(DRAWS, 128).astype(bf16).astype(f32)
        scale = lax.rsqrt(jnp.sum(c * c, axis=0, keepdims=True) / (DRAWS - 1) + EPS)
        u_ref[j * 128 : (j + 1) * 128, :] = (c * scale).T.astype(bf16)
        if j == 0:
            copies = [
                pltpu.make_async_copy(q_ref, q_out.at[i], sem.at[i]) for i in range(16)
            ]
            for copy in copies:
                copy.start()
    for copy in copies:
        copy.wait()


def centre(slots, arr):
    return pl.pallas_call(
        centre_body,
        in_specs=[
            pl.BlockSpec(memory_space=pltpu.SMEM),
            pl.BlockSpec(memory_space=pltpu.VMEM),
        ],
        out_shape=(
            jax.ShapeDtypeStruct((RUN, DRAWS), bf16),
            jax.ShapeDtypeStruct((16, DRAWS, QPIECE), bf16),
        ),
        out_specs=[
            pl.BlockSpec(memory_space=pltpu.VMEM),
            pl.BlockSpec(memory_space=pltpu.HBM),
        ],
        scratch_shapes=[
            pltpu.VMEM((CHAINS, PER_CHAIN, QPIECE), f32),
            pltpu.VMEM((CHAINS, PER_CHAIN, QPIECE), f32),
            pltpu.VMEM((16, 8, 128), f32),
            pltpu.VMEM((DRAWS, QPIECE), bf16),
            pltpu.SemaphoreType.DMA((16,)),
        ],
        compiler_params=params(16),
        name="centre",
    )(slots, arr)


def rows_kept(block, begin, end):
    at = lax.broadcasted_iota(jnp.int32, block.shape, 0)
    inside = (at >= begin) & (at < end)
    return jnp.where(inside, block.astype(f32), 0.0).astype(bf16)


def weights_body(qa_ref, qb_ref, weight_a, weight_b):
    for q_ref, weight_ref in ((qa_ref, weight_a), (qb_ref, weight_b)):
        for i in range(16):
            o = (i % 2 * 8 + i // 2) * QPIECE
            wide = q_ref[i].astype(f32)
            scale = lax.rsqrt(jnp.sum(wide * wide, axis=0, keepdims=True) / (DRAWS - 1) + EPS)
            weight_ref[:, o : o + QPIECE] = (scale / (DRAWS - 1)) * (scale / (DRAWS - 1))


def weights(qa, qb):
    vmem = pl.BlockSpec(memory_space=pltpu.VMEM)
    return pl.pallas_call(
        weights_body,
        in_specs=[vmem] * 2,
        out_shape=[jax.ShapeDtypeStruct((1, NQ_HALF), f32)] * 2,
        out_specs=[vmem] * 2,
        compiler_params=params(16),
        name="weights",
    )(qa, qb)


def docs_body(runs_ref, len_ref, bases_ref, starts_ref, ends_ref, first_ref, main_ref, last_ref):
    lengths = len_ref[...].astype(f32)
    row = lax.broadcasted_iota(jnp.int32, (DOCS, DOCS), 0)
    col = lax.broadcasted_iota(jnp.int32, (DOCS, DOCS), 1)
    column = jnp.sum(jnp.where(row == col, lengths, 0.0), axis=1, keepdims=True)
    ends_column = jnp.sum(jnp.where(col <= row, lengths, 0.0), axis=1, keepdims=True)
    ends = jnp.sum(jnp.where(row <= col, column, 0.0), axis=0, keepdims=True)
    ends_ref[...] = ends.astype(jnp.int32)
    starts_ref[...] = (ends - lengths).astype(jnp.int32)
    group = lax.broadcasted_iota(jnp.int32, (1, NT_HERE // SUB), 1)
    per_run = RUN // SUB
    base = group % per_run * SUB
    for i in range(4):
        base = base + jnp.where(group // per_run == i, runs_ref[i], 0)
    bases_ref[...] = base
    for ref, o in ((first_ref, 0), (main_ref, SUB // 2), (last_ref, SUB - 1)):
        before = ends_column <= (base + o).astype(f32)
        ref[...] = jnp.sum(jnp.where(before, 1.0, 0.0), axis=0, keepdims=True).astype(jnp.int32)


def docs_tables(runs, lengths):
    vmem = pl.BlockSpec(memory_space=pltpu.VMEM)
    groups = jax.ShapeDtypeStruct((1, NT_HERE // SUB), jnp.int32)
    table = jax.ShapeDtypeStruct((1, DOCS), jnp.int32)
    return pl.pallas_call(
        docs_body,
        in_specs=[pl.BlockSpec(memory_space=pltpu.SMEM), vmem],
        out_specs=[vmem] * 6,
        out_shape=[groups, table, table, groups, groups, groups],
        compiler_params=params(16),
        name="docs",
    )(runs, lengths)


def pool_first_body(core_ref, bases_ref, starts_ref, ends_ref, first_ref, main_ref, last_ref,
                    own, left, right, far, q_ref,
                    send_ref, keep_ref, tok, main_tok, qs, acc, *lists):
    i = 0
    for ref in (own, left, right, far):
        for r in range(0, RUN, SUB):
            block = ref[r : r + SUB, :]
            k = main_ref[0, i]
            tok[i * SUB : (i + 1) * SUB, :] = block
            main_tok[i * SUB : (i + 1) * SUB, :] = rows_kept(
                block, starts_ref[0, k] - bases_ref[0, i], ends_ref[0, k] - bases_ref[0, i]
            )
            i += 1
    pool_columns(core_ref, bases_ref, starts_ref, ends_ref, first_ref, main_ref, last_ref,
                 tok, main_tok, q_ref, send_ref, keep_ref, qs, acc, *lists)


def pool_columns(core_ref, bases_ref, starts_ref, ends_ref, first_ref, main_ref, last_ref,
                 tok, main_tok, q_ref, send_ref, keep_ref, qs, acc,
                 picked, sub_list, doc_list):
    core = core_ref[0]
    for i in range(16):
        o = (i % 2 * 8 + i // 2) * QPIECE
        qs[:, o : o + QPIECE] = q_ref[i]
    acc[...] = jnp.zeros_like(acc)

    def row_of(k):
        owner = k // DOC_OWN
        keep = jnp.where(owner % 2 == core, 1, 0)
        return keep * (DOCS // 2) + owner // 2 * DOC_OWN + k % DOC_OWN

    def add_sums(lhs, docs):
        rows = [row_of(k) for k in docs]
        size = lhs.shape[0] // len(rows)
        for b in range(NQ_HALF // NBLK):
            where = slice(b * NBLK, (b + 1) * NBLK)
            s = jnp.dot(lhs, qs[:, where], preferred_element_type=f32)
            p = s * jnp.abs(s)
            for j, row in enumerate(rows):
                acc[pl.ds(row, 1), where] += jnp.sum(
                    p[j * size : (j + 1) * size], axis=0, keepdims=True
                )

    @pl.loop(0, NT_HERE // BODY)
    def _(block):
        for j in range(BODY // TILE):
            i = block * (BODY // TILE) + j
            lhs = main_tok[pl.ds(pl.multiple_of(i * TILE, TILE), TILE), :]
            add_sums(lhs, [main_ref[0, i * (TILE // SUB) + h] for h in range(TILE // SUB)])

    def list_docs(i, n):
        def list_doc(k, n):
            other = k != main_ref[0, i]

            @pl.when(other)
            def _():
                sub_list[n] = i
                doc_list[n] = k

            return n + other.astype(jnp.int32)

        return lax.fori_loop(first_ref[0, i], last_ref[0, i] + 1, list_doc, n)

    extra = lax.fori_loop(0, NT_HERE // SUB, list_docs, 0)
    half = SUB // 2

    @pl.loop(0, (extra + PASSES - 1) // PASSES)
    def _(g):
        docs = []
        for j in range(PASSES):
            e = g * PASSES + j
            at = jnp.minimum(e, extra - 1)
            i = sub_list[at]
            k = doc_list[at]
            o = jnp.where(k > main_ref[0, i], half, 0)
            base = bases_ref[0, i] + o
            end = jnp.where(e < extra, ends_ref[0, k] - base, 0)
            rows = pl.multiple_of(i * SUB + o, half)
            picked[j * half : (j + 1) * half, :] = rows_kept(
                tok[pl.ds(rows, half), :], starts_ref[0, k] - base, end
            )
            docs.append(k)
        add_sums(picked[...], docs)

    send_ref[...] = acc[: DOCS // 2, :]
    keep_ref[...] = acc[DOCS // 2 :, :]


def pool(where, tokens, q):
    smem = pl.BlockSpec(memory_space=pltpu.SMEM)
    vmem = pl.BlockSpec(memory_space=pltpu.VMEM)
    sums = jax.ShapeDtypeStruct((DOCS // 2, NQ_HALF), f32)
    shapes = [sums, sums]
    is_first = len(tokens) == 4
    if is_first:
        shapes += [jax.ShapeDtypeStruct((NT_HERE, DRAWS), bf16)] * 2
    return pl.pallas_call(
        pool_first_body if is_first else pool_columns,
        in_specs=[smem] * len(where) + [vmem] * (len(tokens) + 1),
        out_shape=shapes,
        out_specs=[vmem] * len(shapes),
        scratch_shapes=[
            pltpu.VMEM((DRAWS, NQ_HALF), bf16),
            pltpu.VMEM((DOCS, NQ_HALF), f32),
            pltpu.VMEM((TILE, DRAWS), bf16),
            pltpu.SMEM((DOCS,), jnp.int32),
            pltpu.SMEM((DOCS,), jnp.int32),
        ],
        compiler_params=params(20),
        cost_estimate=pl.CostEstimate(
            flops=2 * NT_HERE * NQ_HALF * DRAWS, bytes_accessed=5 << 20, transcendentals=0
        ),
        name="pool",
    )(*where, *tokens, q)


def combine_body(keep_a, got_a, weight_a, keep_b, got_b, weight_b, out_ref):
    half = NQ_HALF // 2
    for d in range(16):
        ylz, yh = d // 2, d % 2
        r = slice(ylz * DOC_OWN, (ylz + 1) * DOC_OWN)
        c = slice(yh * half, (yh + 1) * half)
        out_ref[d, :, :half] = (keep_a[r, c] + got_a[r, c]) * weight_a[:, c]
        out_ref[d, :, half:] = (keep_b[r, c] + got_b[r, c]) * weight_b[:, c]


def combine(*arrays):
    return pl.pallas_call(
        combine_body,
        in_specs=[pl.BlockSpec(memory_space=pltpu.VMEM)] * 6,
        out_specs=pl.BlockSpec(memory_space=pltpu.VMEM),
        out_shape=jax.ShapeDtypeStruct((16, DOC_OWN, NQ_HALF), f32),
        compiler_params=params(16),
        name="combine",
    )(*arrays)


def finish_body(core_ref, total_ref, len_ref, out_ref):
    core = core_ref[0]
    total = total_ref[...] / len_ref[...]
    for k, c in enumerate((core, 1 - core)):
        for ylz in range(8):
            o = pl.multiple_of((ylz * 2 + c) * QPIECE, QPIECE)
            i = (k * 8 + ylz) * QPIECE
            out_ref[:, pl.ds(o, QPIECE)] = total[:, i : i + QPIECE]


def finish(core, total, lengths):
    vmem = pl.BlockSpec(memory_space=pltpu.VMEM)
    return pl.pallas_call(
        finish_body,
        in_specs=[pl.BlockSpec(memory_space=pltpu.SMEM)] + [vmem] * 2,
        out_specs=vmem,
        out_shape=jax.ShapeDtypeStruct((DOC_OWN, NQ_HALF), f32),
        compiler_params=params(16),
        name="finish",
    )(core, total, lengths)


def shift(value, axis, by):
    size = lax.axis_size(axis)
    return lax.ppermute(value, axis, [(i, (i + by) % size) for i in range(size)])


def step(train_losses, query_losses, chain_slots, doc_lengths):
    core = lax.axis_index("c")
    yh = lax.axis_index("yh")
    x = lax.axis_index("x")
    t = (lax.axis_index("yl") * 4 + lax.axis_index("z")) * 2 + core

    packed = pack(train_losses, query_losses)
    arrived = lax.all_to_all(packed, ("yl", "z", "c"), split_axis=0, concat_axis=0, tiled=True)
    own, copies = centre(chain_slots, arrived)

    left = shift(own, "x", 1)
    right = shift(own, "x", -1)
    far_lo = shift(left[: RUN // 2], "x", 1)
    far_hi = shift(right[RUN // 2 :], "x", -1)
    far = jnp.concatenate([far_lo, far_hi])

    qa = lax.all_to_all(copies, ("yl", "z", "yh"), split_axis=0, concat_axis=0, tiled=True)
    qb = shift(qa, "c", 1)

    xs = jnp.stack([x, (x + 3) % 4, (x + 1) % 4, (x + 2) % 4])
    runs = (xs * 2 + yh) * (16 * RUN) + t * RUN
    tables = docs_tables(runs, doc_lengths.reshape(1, DOCS))
    bases, doc_starts, doc_ends, first, main, last = tables

    where = (core.reshape(1), bases, doc_starts, doc_ends, first, main, last)
    send_a, keep_a, tok, main_tok = pool(where, (own, left, right, far), qa)
    cross_a = shift(send_a, "c", 1)
    send_b, keep_b = pool(where, (tok, main_tok), qb)
    cross_b = shift(send_b, "c", 1)
    weight_a, weight_b = weights(qa, qb)
    sums = combine(keep_a, cross_b, weight_a, keep_b, cross_a, weight_b)
    pieces = lax.all_to_all(
        sums.astype(jnp.float16), ("yl", "z", "yh"), split_axis=0, concat_axis=0, tiled=True
    )
    total = jnp.sum(pieces.astype(f32), axis=0)
    lengths = lax.dynamic_slice_in_dim(doc_lengths, t * DOC_OWN, DOC_OWN, 0).astype(f32)
    return finish(core.reshape(1), total, lengths[:, None])


def solution(mesh):
    fine = Mesh(mesh.devices.reshape(2, 4, 2, 4, 2), ("yl", "z", "c", "x", "yh"))
    split = P(("yl", "z", "c"), ("x", "yh"))
    return jax.shard_map(
        step, mesh=fine, in_specs=(split, split, P(), P()), out_specs=split, check_vma=False
    )
```

```python
import jax
import jax.numpy as jnp
from jax import lax
from jax.experimental import pallas as pl
from jax.experimental.pallas import tpu as pltpu
from jax.sharding import Mesh
from jax.sharding import PartitionSpec as P

DRAWS = 256
CHAINS = 32
PER_CHAIN = DRAWS // CHAINS
EPS = 1e-06
DOCS = 128
DOC_OWN = 8
RUN = 1024
QPIECE = 128
TILE = 256
SUB = 128
PASSES = TILE // (SUB // 2)
NBLK = 512
BODY = 2048
PACK_MIB = 62
NQ_HALF = 2048
PIECE = RUN + 256 + 2 * QPIECE
NT_HERE = 4096

f32 = jnp.float32
bf16 = jnp.bfloat16


def params(mib=48):
    return pltpu.CompilerParams(vmem_limit_bytes=mib * 1024 * 1024)


def terms(value):
    hi = value.astype(bf16).astype(f32)
    rest = value - hi
    mid = rest.astype(bf16).astype(f32)
    return hi, mid, rest - mid


def pack_body(train_hbm, query_hbm, out_hbm, train_ref, query_ref, out_ref, sem, out_sem):
    width = train_ref.shape[1] // 4
    copies = [pltpu.make_async_copy(query_hbm, query_ref, sem.at[4])]
    for i in range(4):
        cols = pl.ds(i * width, width)
        copies.append(pltpu.make_async_copy(train_hbm.at[:, cols], train_ref.at[:, cols], sem.at[i]))
    for copy in copies:
        copy.start()
    out_copies = []
    for i in range(4):
        part = pl.ds(i * 4, 4)
        out_copies.append(pltpu.make_async_copy(out_ref.at[part], out_hbm.at[part], out_sem.at[i]))
    copies[0].wait()
    rows = train_ref.shape[0]
    for i in range(16):
        if i % 4 == 0:
            copies[1 + i // 4].wait()
        if i % 4 == 1 and i > 4:
            out_copies[i // 4 - 1].start()
        block = train_ref[:, i * RUN : (i + 1) * RUN]
        mean = jnp.sum(block, axis=0, keepdims=True) / rows
        out_ref[i, :, :RUN] = (block - mean).astype(bf16)
        stacked = jnp.concatenate([mean[:, j * 128 : (j + 1) * 128] for j in range(8)], axis=0)
        hi, mid, lo = terms(stacked)
        block = query_ref[:, i * QPIECE : (i + 1) * QPIECE]
        mean = jnp.sum(block, axis=0, keepdims=True) / rows
        means = terms(mean)
        low = jnp.concatenate([lo, *means, jnp.zeros((5, 128), f32)], axis=0)
        o = RUN
        out_ref[i, :, o : o + 128] = jnp.concatenate([hi, mid], axis=0).astype(bf16)
        out_ref[i, :, o + 128 : o + 256] = low.astype(bf16)
        hi, mid, _ = terms(block - mean)
        out_ref[i, :, o + 256 : o + 384] = hi.astype(bf16)
        out_ref[i, :, o + 384 : o + 512] = mid.astype(bf16)
    out_copies[3].start()
    for copy in out_copies:
        copy.wait()


def pack(train, query):
    return pl.pallas_call(
        pack_body,
        in_specs=[pl.BlockSpec(memory_space=pltpu.HBM)] * 2,
        out_specs=pl.BlockSpec(memory_space=pltpu.HBM),
        out_shape=jax.ShapeDtypeStruct((16, train.shape[0], PIECE), bf16),
        scratch_shapes=[
            pltpu.VMEM(train.shape, f32),
            pltpu.VMEM(query.shape, f32),
            pltpu.VMEM((16, train.shape[0], PIECE), bf16),
            pltpu.SemaphoreType.DMA((5,)),
            pltpu.SemaphoreType.DMA((4,)),
        ],
        compiler_params=params(PACK_MIB),
        name="pack",
    )(train, query)


def centre_body(slots_ref, arr_ref, u_ref, q_out, qc_ref, qp_ref, mean_ref, q_ref, sem):
    def part(o):
        return arr_ref[:, :, o : o + 128].astype(f32)

    low = part(RUN + 128)
    local = (low[:, 10:11] + low[:, 9:10]) + low[:, 8:9]
    offset = local - jnp.sum(local, axis=0, keepdims=True) / 16
    query = (part(RUN + 384) + part(RUN + 256)) + offset
    qc = query.reshape(DRAWS, QPIECE).astype(bf16).astype(f32)
    qc_ref[...] = qc.reshape(CHAINS, PER_CHAIN, QPIECE)
    for s in range(CHAINS):
        qp_ref[s] = qc_ref[slots_ref[s]]
    q_ref[...] = qp_ref[...].reshape(DRAWS, QPIECE).astype(bf16)

    upper = part(RUN)
    mean_ref[...] = (low[:, :8] + upper[:, 8:]) + upper[:, :8]
    for j in range(RUN // 128):
        local = mean_ref[:, j : j + 1, :]
        offset = local - jnp.sum(local, axis=0, keepdims=True) / 16
        c = (part(j * 128) + offset).reshape(DRAWS, 128).astype(bf16).astype(f32)
        scale = lax.rsqrt(jnp.sum(c * c, axis=0, keepdims=True) / (DRAWS - 1) + EPS)
        u_ref[j * 128 : (j + 1) * 128, :] = (c * scale).T.astype(bf16)
        if j == 0:
            copies = [
                pltpu.make_async_copy(q_ref, q_out.at[i], sem.at[i]) for i in range(16)
            ]
            for copy in copies:
                copy.start()
    for copy in copies:
        copy.wait()


def centre(slots, arr):
    return pl.pallas_call(
        centre_body,
        in_specs=[
            pl.BlockSpec(memory_space=pltpu.SMEM),
            pl.BlockSpec(memory_space=pltpu.VMEM),
        ],
        out_shape=(
            jax.ShapeDtypeStruct((RUN, DRAWS), bf16),
            jax.ShapeDtypeStruct((16, DRAWS, QPIECE), bf16),
        ),
        out_specs=[
            pl.BlockSpec(memory_space=pltpu.VMEM),
            pl.BlockSpec(memory_space=pltpu.HBM),
        ],
        scratch_shapes=[
            pltpu.VMEM((CHAINS, PER_CHAIN, QPIECE), f32),
            pltpu.VMEM((CHAINS, PER_CHAIN, QPIECE), f32),
            pltpu.VMEM((16, 8, 128), f32),
            pltpu.VMEM((DRAWS, QPIECE), bf16),
            pltpu.SemaphoreType.DMA((16,)),
        ],
        compiler_params=params(16),
        name="centre",
    )(slots, arr)


def rows_kept(block, begin, end):
    at = lax.broadcasted_iota(jnp.int32, block.shape, 0)
    inside = (at >= begin) & (at < end)
    return jnp.where(inside, block.astype(f32), 0.0).astype(bf16)


def weights_body(qa_ref, qb_ref, weight_a, weight_b):
    for q_ref, weight_ref in ((qa_ref, weight_a), (qb_ref, weight_b)):
        for i in range(16):
            o = (i % 2 * 8 + i // 2) * QPIECE
            wide = q_ref[i].astype(f32)
            scale = lax.rsqrt(jnp.sum(wide * wide, axis=0, keepdims=True) / (DRAWS - 1) + EPS)
            weight_ref[:, o : o + QPIECE] = (scale / (DRAWS - 1)) * (scale / (DRAWS - 1))


def weights(qa, qb):
    vmem = pl.BlockSpec(memory_space=pltpu.VMEM)
    return pl.pallas_call(
        weights_body,
        in_specs=[vmem] * 2,
        out_shape=[jax.ShapeDtypeStruct((1, NQ_HALF), f32)] * 2,
        out_specs=[vmem] * 2,
        compiler_params=params(16),
        name="weights",
    )(qa, qb)


def touch_body(lo_ref, hi_ref, out_ref):
    out_ref[...] = (lo_ref[:8, :].astype(f32) + hi_ref[:8, :].astype(f32))[:1, :128]


def touch(lo, hi):
    rows = pl.BlockSpec((16, DRAWS), lambda i: (0, 0))
    return pl.pallas_call(
        touch_body,
        grid=(1,),
        in_specs=[rows] * 2,
        out_specs=pl.BlockSpec((1, 128), lambda i: (0, 0)),
        out_shape=jax.ShapeDtypeStruct((1, 128), f32),
        compiler_params=params(4),
        name="touch",
    )(lo, hi)


def docs_body(runs_ref, len_ref, bases_ref, starts_ref, ends_ref, first_ref, main_ref, last_ref):
    lengths = len_ref[...].astype(f32)
    row = lax.broadcasted_iota(jnp.int32, (DOCS, DOCS), 0)
    col = lax.broadcasted_iota(jnp.int32, (DOCS, DOCS), 1)
    column = jnp.sum(jnp.where(row == col, lengths, 0.0), axis=1, keepdims=True)
    ends_column = jnp.sum(jnp.where(col <= row, lengths, 0.0), axis=1, keepdims=True)
    ends = jnp.sum(jnp.where(row <= col, column, 0.0), axis=0, keepdims=True)
    ends_ref[...] = ends.astype(jnp.int32)
    starts_ref[...] = (ends - lengths).astype(jnp.int32)
    group = lax.broadcasted_iota(jnp.int32, (1, NT_HERE // SUB), 1)
    per_run = RUN // SUB
    base = group % per_run * SUB
    for i in range(4):
        base = base + jnp.where(group // per_run == i, runs_ref[i], 0)
    bases_ref[...] = base
    for ref, o in ((first_ref, 0), (main_ref, SUB // 2), (last_ref, SUB - 1)):
        before = ends_column <= (base + o).astype(f32)
        ref[...] = jnp.sum(jnp.where(before, 1.0, 0.0), axis=0, keepdims=True).astype(jnp.int32)


def docs_tables(runs, lengths):
    vmem = pl.BlockSpec(memory_space=pltpu.VMEM)
    groups = jax.ShapeDtypeStruct((1, NT_HERE // SUB), jnp.int32)
    table = jax.ShapeDtypeStruct((1, DOCS), jnp.int32)
    return pl.pallas_call(
        docs_body,
        in_specs=[pl.BlockSpec(memory_space=pltpu.SMEM), vmem],
        out_specs=[vmem] * 6,
        out_shape=[groups, table, table, groups, groups, groups],
        compiler_params=params(16),
        name="docs",
    )(runs, lengths)


def pool_first_body(seen_ref, core_ref, bases_ref, starts_ref, ends_ref, first_ref, main_ref, last_ref,
                    own, left, right, far_lo, far_hi, q_ref,
                    send_ref, keep_ref, tok, main_tok, qs, acc, *lists):
    i = 0
    for ref in (own, left, right, far_lo, far_hi):
        for r in range(0, ref.shape[0], SUB):
            block = ref[r : r + SUB, :]
            k = main_ref[0, i]
            tok[i * SUB : (i + 1) * SUB, :] = block
            main_tok[i * SUB : (i + 1) * SUB, :] = rows_kept(
                block, starts_ref[0, k] - bases_ref[0, i], ends_ref[0, k] - bases_ref[0, i]
            )
            i += 1
    pool_columns(seen_ref, core_ref, bases_ref, starts_ref, ends_ref, first_ref, main_ref, last_ref,
                 tok, main_tok, q_ref, send_ref, keep_ref, qs, acc, *lists)


def pool_columns(seen_ref, core_ref, bases_ref, starts_ref, ends_ref, first_ref, main_ref, last_ref,
                 tok, main_tok, q_ref, send_ref, keep_ref, qs, acc,
                 picked, sub_list, doc_list):
    core = core_ref[0]
    for i in range(16):
        o = (i % 2 * 8 + i // 2) * QPIECE
        qs[:, o : o + QPIECE] = q_ref[i]
    acc[...] = jnp.zeros_like(acc)

    def row_of(k):
        owner = k // DOC_OWN
        keep = jnp.where(owner % 2 == core, 1, 0)
        return keep * (DOCS // 2) + owner // 2 * DOC_OWN + k % DOC_OWN

    def add_sums(lhs, docs):
        rows = [row_of(k) for k in docs]
        size = lhs.shape[0] // len(rows)
        for b in range(NQ_HALF // NBLK):
            where = slice(b * NBLK, (b + 1) * NBLK)
            s = jnp.dot(lhs, qs[:, where], preferred_element_type=f32)
            p = s * jnp.abs(s)
            for j, row in enumerate(rows):
                acc[pl.ds(row, 1), where] += jnp.sum(
                    p[j * size : (j + 1) * size], axis=0, keepdims=True
                )

    @pl.loop(0, NT_HERE // BODY)
    def _(block):
        for j in range(BODY // TILE):
            i = block * (BODY // TILE) + j
            lhs = main_tok[pl.ds(pl.multiple_of(i * TILE, TILE), TILE), :]
            add_sums(lhs, [main_ref[0, i * (TILE // SUB) + h] for h in range(TILE // SUB)])

    def list_docs(i, n):
        def list_doc(k, n):
            other = k != main_ref[0, i]

            @pl.when(other)
            def _():
                sub_list[n] = i
                doc_list[n] = k

            return n + other.astype(jnp.int32)

        return lax.fori_loop(first_ref[0, i], last_ref[0, i] + 1, list_doc, n)

    extra = lax.fori_loop(0, NT_HERE // SUB, list_docs, 0)
    half = SUB // 2

    @pl.loop(0, (extra + PASSES - 1) // PASSES)
    def _(g):
        docs = []
        for j in range(PASSES):
            e = g * PASSES + j
            at = jnp.minimum(e, extra - 1)
            i = sub_list[at]
            k = doc_list[at]
            o = jnp.where(k > main_ref[0, i], half, 0)
            base = bases_ref[0, i] + o
            end = jnp.where(e < extra, ends_ref[0, k] - base, 0)
            rows = pl.multiple_of(i * SUB + o, half)
            picked[j * half : (j + 1) * half, :] = rows_kept(
                tok[pl.ds(rows, half), :], starts_ref[0, k] - base, end
            )
            docs.append(k)
        add_sums(picked[...], docs)

    send_ref[...] = acc[: DOCS // 2, :]
    keep_ref[...] = acc[DOCS // 2 :, :]


def pool(where, tokens, q):
    smem = pl.BlockSpec(memory_space=pltpu.SMEM)
    vmem = pl.BlockSpec(memory_space=pltpu.VMEM)
    sums = jax.ShapeDtypeStruct((DOCS // 2, NQ_HALF), f32)
    shapes = [sums, sums]
    is_first = len(tokens) == 5
    if is_first:
        shapes += [jax.ShapeDtypeStruct((NT_HERE, DRAWS), bf16)] * 2
    return pl.pallas_call(
        pool_first_body if is_first else pool_columns,
        in_specs=[smem] * len(where) + [vmem] * (len(tokens) + 1),
        out_shape=shapes,
        out_specs=[vmem] * len(shapes),
        scratch_shapes=[
            pltpu.VMEM((DRAWS, NQ_HALF), bf16),
            pltpu.VMEM((DOCS, NQ_HALF), f32),
            pltpu.VMEM((TILE, DRAWS), bf16),
            pltpu.SMEM((DOCS,), jnp.int32),
            pltpu.SMEM((DOCS,), jnp.int32),
        ],
        compiler_params=params(20),
        cost_estimate=pl.CostEstimate(
            flops=2 * NT_HERE * NQ_HALF * DRAWS, bytes_accessed=5 << 20, transcendentals=0
        ),
        name="pool",
    )(*where, *tokens, q)


def combine_body(keep_a, got_a, weight_a, keep_b, got_b, weight_b, out_ref):
    half = NQ_HALF // 2
    for d in range(16):
        ylz, yh = d // 2, d % 2
        r = slice(ylz * DOC_OWN, (ylz + 1) * DOC_OWN)
        c = slice(yh * half, (yh + 1) * half)
        out_ref[d, :, :half] = (keep_a[r, c] + got_a[r, c]) * weight_a[:, c]
        out_ref[d, :, half:] = (keep_b[r, c] + got_b[r, c]) * weight_b[:, c]


def combine(*arrays):
    return pl.pallas_call(
        combine_body,
        in_specs=[pl.BlockSpec(memory_space=pltpu.VMEM)] * 6,
        out_specs=pl.BlockSpec(memory_space=pltpu.VMEM),
        out_shape=jax.ShapeDtypeStruct((16, DOC_OWN, NQ_HALF), f32),
        compiler_params=params(16),
        name="combine",
    )(*arrays)


def finish_body(core_ref, total_ref, len_ref, out_ref):
    core = core_ref[0]
    total = total_ref[...] / len_ref[...]
    for k, c in enumerate((core, 1 - core)):
        for ylz in range(8):
            o = pl.multiple_of((ylz * 2 + c) * QPIECE, QPIECE)
            i = (k * 8 + ylz) * QPIECE
            out_ref[:, pl.ds(o, QPIECE)] = total[:, i : i + QPIECE]


def finish(core, total, lengths):
    vmem = pl.BlockSpec(memory_space=pltpu.VMEM)
    return pl.pallas_call(
        finish_body,
        in_specs=[pl.BlockSpec(memory_space=pltpu.SMEM)] + [vmem] * 2,
        out_specs=vmem,
        out_shape=jax.ShapeDtypeStruct((DOC_OWN, NQ_HALF), f32),
        compiler_params=params(16),
        name="finish",
    )(core, total, lengths)


def shift(value, axis, by):
    size = lax.axis_size(axis)
    return lax.ppermute(value, axis, [(i, (i + by) % size) for i in range(size)])


def step(train_losses, query_losses, chain_slots, doc_lengths):
    core = lax.axis_index("c")
    yh = lax.axis_index("yh")
    x = lax.axis_index("x")
    t = (lax.axis_index("yl") * 4 + lax.axis_index("z")) * 2 + core

    packed = pack(train_losses, query_losses)
    arrived = lax.all_to_all(packed, ("yl", "z", "c"), split_axis=0, concat_axis=0, tiled=True)
    own, copies = centre(chain_slots, arrived)

    left = shift(own, "x", 1)
    right = shift(own, "x", -1)
    far_lo = shift(left[: RUN // 2], "x", 1)
    far_hi = shift(right[RUN // 2 :], "x", -1)
    arrived_both = touch(far_lo, far_hi)

    qa = lax.all_to_all(copies, ("yl", "z", "yh"), split_axis=0, concat_axis=0, tiled=True)
    qb = shift(qa, "c", 1)

    xs = jnp.stack([x, (x + 3) % 4, (x + 1) % 4, (x + 2) % 4])
    runs = (xs * 2 + yh) * (16 * RUN) + t * RUN
    tables = docs_tables(runs, doc_lengths.reshape(1, DOCS))
    bases, doc_starts, doc_ends, first, main, last = tables

    where = (arrived_both, core.reshape(1), bases, doc_starts, doc_ends, first, main, last)
    send_a, keep_a, tok, main_tok = pool(where, (own, left, right, far_lo, far_hi), qa)
    cross_a = shift(send_a, "c", 1)
    send_b, keep_b = pool(where, (tok, main_tok), qb)
    cross_b = shift(send_b, "c", 1)
    weight_a, weight_b = weights(qa, qb)
    sums = combine(keep_a, cross_b, weight_a, keep_b, cross_a, weight_b)
    pieces = lax.all_to_all(
        sums.astype(jnp.float16), ("yl", "z", "yh"), split_axis=0, concat_axis=0, tiled=True
    )
    total = jnp.sum(pieces.astype(f32), axis=0)
    lengths = lax.dynamic_slice_in_dim(doc_lengths, t * DOC_OWN, DOC_OWN, 0).astype(f32)
    return finish(core.reshape(1), total, lengths[:, None])


def solution(mesh):
    fine = Mesh(mesh.devices.reshape(2, 4, 2, 4, 2), ("yl", "z", "c", "x", "yh"))
    split = P(("yl", "z", "c"), ("x", "yh"))
    return jax.shard_map(
        step, mesh=fine, in_specs=(split, split, P(), P()), out_specs=split, check_vma=False
    )
```
